16 devices in a mesh: dp: 2 (over y, z), tp: 8 (over x, core).
Axes of the slice: x: 4, y: 2, z: 1, core: 2. Of those that a mesh axis runs over, the one named last changes fastest.
The devices are a block of a 4x4x8 slice.
Arguments:
- x_in: bfloat16 [256, 7168], P('dp'), parts along dimension 0
- pos_ids: int32 [256], P('dp'), parts along dimension 0
- ckv_cache: bfloat16 [2, 256, 128, 512], P(None, 'dp'), parts along dimension 1
- kpe_cache: bfloat16 [2, 256, 128, 64], P(None, 'dp'), parts along dimension 1
- attn_gain: bfloat16 [2, 7168], replicated
- w_dq: bfloat16 [2, 7168, 1536], replicated
- q_gain: bfloat16 [2, 1536], replicated
- w_dkv: bfloat16 [2, 7168, 576], replicated
- kv_gain: bfloat16 [2, 512], replicated
- w_uq: bfloat16 [2, 1536, 32, 192], P(None, None, 'tp')
- w_uk: bfloat16 [2, 512, 32, 128], P(None, None, 'tp')
- w_uv: bfloat16 [2, 512, 32, 128], P(None, None, 'tp')
- w_o: bfloat16 [2, 32, 128, 7168], P(None, 'tp')
- mlp_gain: bfloat16 [2, 7168], replicated
- w_gate: bfloat16 [2, 7168, 4608], P(None, None, 'tp')
- w_up: bfloat16 [2, 7168, 4608], P(None, None, 'tp')
- w_down: bfloat16 [2, 4608, 7168], P(None, 'tp')
Outputs:
- output 1: bfloat16 [256, 7168], P('dp'), parts along dimension 0
- output 2: bfloat16 [2, 256, 512], P(None, 'dp'), parts along dimension 1
- output 3: bfloat16 [2, 256, 64], P(None, 'dp'), parts along dimension 1
There are 2 independent parts. The reference program is written for one: setup_inputs(seed, part) draws one part's arguments, and reference() takes and returns one part's arrays. A program takes and returns all parts, laid end to end along the dimension named above; an argument that names none is the same for every part.
All inputs are finite; a program needn't handle non-finite values.
Results may differ from the reference program's by a relative error of at most 0.02.
Values are sent between devices in bfloat16 or wider.
A program may use at most 768 MiB of HBM per device.

```python
import math
import jax
import jax.numpy as jnp
from jax import lax

SEQ_COUNT = 128
CACHE_LEN = 128
MODEL_DIM = 7168
FFN_DIM = 4608
NUM_HEADS = 32
Q_LORA = 1536
KV_LORA = 512
ROPE_DIM = 64
NOPE_DIM = 128
VALUE_DIM = 128
LAYER_COUNT = 2
ROPE_BASE = 10000

NORM_EPS = 1e-6
SCORE_SCALE = (NOPE_DIM + ROPE_DIM) ** -0.5


def rms_norm(values, norm_gain):
    values = values.astype(jnp.float32)
    inv_rms = lax.rsqrt(jnp.mean(values * values, axis=-1, keepdims=True) + NORM_EPS)
    return (values * inv_rms * norm_gain.astype(jnp.float32)).astype(jnp.bfloat16)


def rotary(values, positions):
    half_dim = ROPE_DIM // 2
    inv_freq = jnp.exp(jnp.arange(half_dim, dtype=jnp.float32) * (-2.0 * math.log(ROPE_BASE) / ROPE_DIM))
    angles = positions.astype(jnp.float32)[..., None] * inv_freq
    cos_part = jnp.cos(angles)
    sin_part = jnp.sin(angles)
    lo_half = values[..., :half_dim]
    hi_half = values[..., half_dim:]
    return jnp.concatenate([lo_half * cos_part - hi_half * sin_part, hi_half * cos_part + lo_half * sin_part], axis=-1)


def draw_normal(key, shape, std_dev):
    return (jax.random.normal(key, shape, jnp.float32) * std_dev).astype(jnp.bfloat16)


def draw_gain(key, width):
    return (1.0 + 0.25 * jax.random.normal(key, (LAYER_COUNT, width), jnp.float32)).astype(jnp.bfloat16)


def setup_inputs(seed: int = 0, part: int = 0) -> dict:
    shared_keys = jax.random.split(jax.random.key(seed), 16)
    local_keys = jax.random.split(jax.random.fold_in(jax.random.key(seed + 1), part), 6)
    qk_dim = NOPE_DIM + ROPE_DIM
    low_pos = CACHE_LEN // 2
    pos_ids = jax.random.randint(local_keys[1], (SEQ_COUNT,), low_pos, CACHE_LEN, jnp.int32)
    pos_ids = pos_ids.at[0].set(CACHE_LEN - 1).at[1].set(low_pos)
    seq_mean = jax.random.normal(local_keys[2], (LAYER_COUNT, SEQ_COUNT, 1, KV_LORA), jnp.float32)
    cache_noise = jax.random.normal(local_keys[3], (LAYER_COUNT, SEQ_COUNT, CACHE_LEN, KV_LORA), jnp.float32)
    return {
        'x_in': draw_normal(local_keys[0], (SEQ_COUNT, MODEL_DIM), 1.0),
        'pos_ids': pos_ids,
        'ckv_cache': (0.8 * seq_mean + 0.6 * cache_noise).astype(jnp.bfloat16),
        'kpe_cache': draw_normal(local_keys[4], (LAYER_COUNT, SEQ_COUNT, CACHE_LEN, ROPE_DIM), 1.0),
        'attn_gain': draw_gain(shared_keys[0], MODEL_DIM),
        'w_dq': draw_normal(shared_keys[1], (LAYER_COUNT, MODEL_DIM, Q_LORA), MODEL_DIM ** -0.5),
        'q_gain': draw_gain(shared_keys[2], Q_LORA),
        'w_dkv': draw_normal(shared_keys[3], (LAYER_COUNT, MODEL_DIM, KV_LORA + ROPE_DIM), MODEL_DIM ** -0.5),
        'kv_gain': draw_gain(shared_keys[4], KV_LORA),
        'w_uq': draw_normal(shared_keys[5], (LAYER_COUNT, Q_LORA, NUM_HEADS, qk_dim), Q_LORA ** -0.5),
        'w_uk': draw_normal(shared_keys[6], (LAYER_COUNT, KV_LORA, NUM_HEADS, NOPE_DIM), 3.0 * NOPE_DIM ** -0.5),
        'w_uv': draw_normal(shared_keys[7], (LAYER_COUNT, KV_LORA, NUM_HEADS, VALUE_DIM), KV_LORA ** -0.5),
        'w_o': draw_normal(shared_keys[8], (LAYER_COUNT, NUM_HEADS, VALUE_DIM, MODEL_DIM), (NUM_HEADS * VALUE_DIM) ** -0.5),
        'mlp_gain': draw_gain(shared_keys[9], MODEL_DIM),
        'w_gate': draw_normal(shared_keys[10], (LAYER_COUNT, MODEL_DIM, FFN_DIM), MODEL_DIM ** -0.5),
        'w_up': draw_normal(shared_keys[11], (LAYER_COUNT, MODEL_DIM, FFN_DIM), MODEL_DIM ** -0.5),
        'w_down': draw_normal(shared_keys[12], (LAYER_COUNT, FFN_DIM, MODEL_DIM), FFN_DIM ** -0.5),
    }


def attend_one(seq_item):
    q_lat, q_rope, ckv_seq, kpe_seq, position = seq_item
    scores = jnp.dot(q_lat, ckv_seq.T, preferred_element_type=jnp.float32)
    scores = (scores + jnp.dot(q_rope, kpe_seq.T, preferred_element_type=jnp.float32)) * SCORE_SCALE
    visible = jnp.arange(CACHE_LEN)[None, :] <= position
    scores = jnp.where(visible, scores, -jnp.inf)
    attn_prob = jax.nn.softmax(scores, axis=-1).astype(jnp.bfloat16)
    return jnp.dot(attn_prob, ckv_seq, preferred_element_type=jnp.float32).astype(jnp.bfloat16)


def one_layer(hidden, pos_ids, layer_in):
    (ckv_old, kpe_old, attn_gain, w_dq, q_gain, w_dkv, kv_gain, w_uq, w_uk, w_uv, w_o, mlp_gain, w_gate, w_up, w_down) = layer_in
    normed = rms_norm(hidden, attn_gain)
    c_q = rms_norm(jnp.dot(normed, w_dq, preferred_element_type=jnp.float32), q_gain)
    q_full = jnp.einsum('bc,chd->bhd', c_q.astype(jnp.float32), w_uq.astype(jnp.float32))
    q_nope = q_full[..., :NOPE_DIM].astype(jnp.bfloat16)
    q_rope = rotary(q_full[..., NOPE_DIM:], pos_ids[:, None]).astype(jnp.bfloat16)
    q_lat = jnp.einsum('bhn,chn->bhc', q_nope.astype(jnp.float32), w_uk.astype(jnp.float32)).astype(jnp.bfloat16)
    kv_lat = jnp.dot(normed, w_dkv, preferred_element_type=jnp.float32)
    ckv_new = rms_norm(kv_lat[:, :KV_LORA], kv_gain)
    kpe_new = rotary(kv_lat[:, KV_LORA:], pos_ids).astype(jnp.bfloat16)
    at_pos = (jnp.arange(CACHE_LEN)[None, :] == pos_ids[:, None])[:, :, None]
    ckv_all = jnp.where(at_pos, ckv_new[:, None, :], ckv_old)
    kpe_all = jnp.where(at_pos, kpe_new[:, None, :], kpe_old)
    context = lax.map(attend_one, (q_lat, q_rope, ckv_all, kpe_all, pos_ids))
    head_out = jnp.einsum('bhc,chv->bhv', context.astype(jnp.float32), w_uv.astype(jnp.float32)).astype(jnp.bfloat16)
    attn_sum = jnp.einsum('bhv,hvd->bd', head_out.astype(jnp.float32), w_o.astype(jnp.float32))
    mid_state = (hidden.astype(jnp.float32) + attn_sum).astype(jnp.bfloat16)
    mlp_in = rms_norm(mid_state, mlp_gain)
    gate_pre = jnp.dot(mlp_in, w_gate, preferred_element_type=jnp.float32)
    up_pre = jnp.dot(mlp_in, w_up, preferred_element_type=jnp.float32)
    act_out = (jax.nn.silu(gate_pre) * up_pre).astype(jnp.bfloat16)
    mlp_sum = jnp.dot(act_out, w_down, preferred_element_type=jnp.float32)
    layer_out = (mid_state.astype(jnp.float32) + mlp_sum).astype(jnp.bfloat16)
    return layer_out, (ckv_new, kpe_new)


def reference(x_in, pos_ids, ckv_cache, kpe_cache, attn_gain, w_dq, q_gain, w_dkv, kv_gain, w_uq, w_uk, w_uv, w_o, mlp_gain, w_gate, w_up, w_down):
    def layer_step(hidden, layer_in):
        return one_layer(hidden, pos_ids, layer_in)
    stacked = (ckv_cache, kpe_cache, attn_gain, w_dq, q_gain, w_dkv, kv_gain, w_uq, w_uk, w_uv, w_o, mlp_gain, w_gate, w_up, w_down)
    x_out, (ckv_rows, kpe_rows) = lax.scan(layer_step, x_in, stacked)
    return x_out, ckv_rows, kpe_rows
```

```python
import math
import functools
import jax
import jax.numpy as jnp
from jax import lax
from jax.experimental import pallas as pl
from jax.experimental.pallas import tpu as pltpu
from jax.sharding import PartitionSpec as P

NORM_EPS = 1e-6
ROPE_BASE = 10000.0
F32 = jnp.float32
BF16 = jnp.bfloat16
MESH = pl.DeviceIdType.MESH
NEG_INF = float('-inf')


def rms(values, gain):
    inv = lax.rsqrt(jnp.mean(values * values, axis=-1, keepdims=True) + NORM_EPS)
    return values * inv * gain


def dot_nt(lhs, rhs):
    return lax.dot_general(lhs, rhs, (((1,), (1,)), ((), ())), preferred_element_type=F32)


def dot_nn(lhs, rhs):
    return jnp.dot(lhs, rhs, preferred_element_type=F32)


def swap_halves(values, half):
    width = values.shape[-1]
    lane = lax.broadcasted_iota(jnp.int32, values.shape, 1)
    up = pltpu.roll(values, half, 1)
    down = pltpu.roll(values, width - half, 1)
    return jnp.where(lane % (2 * half) < half, down, up)


def tile_rows(values, count):
    return jnp.concatenate([values] * count, axis=0)


def step_kernel(cfg, x_hbm, cos_ref, sin_ref, pos_ref, ag_ref, mg_ref, qg_ref, kg_ref,
                wdq, wkv, wuq, wuk, wuv, wo, wg, wu, wd, ckv_hbm, kpe_hbm,
                x_out, ckv_out, kpe_out,
                xb, a_buf, b_all, q_all, acc_q, acc_kv, u_buf, r_buf, ctx_buf, o_buf, wf,
                gate_acc, up_acc, act_buf,
                part, d2d, psum, rel, cmb, fin,
                dq_buf, kv_buf, uq_buf, uk_buf, uv_buf, wo_buf, wg_buf, wu_buf, wd_buf, ckv_buf, kpe_buf,
                x_sem, dq_sem, kv_sem, w_sem, c_sem, out_sem,
                ag_send, ag_recv, rs_send, rs_recv):
    tp_size, layers, heads, kc, slots, chunks, seqs = (
        cfg['tp'], cfg['layers'], cfg['heads'], cfg['kc'], cfg['slots'], cfg['chunks'], cfg['seqs'])
    nchip = tp_size // 2
    model = xb.shape[1]
    rows = xb.shape[0]
    lora = uq_buf.shape[1]
    latent = ckv_buf.shape[-1]
    rope = kpe_buf.shape[2]
    nope = uk_buf.shape[1]
    keys = ckv_buf.shape[2]
    batch = rows * tp_size
    n_dq = model // kc
    cw = model // chunks
    ch = cw // 2
    scale = float((nope + rope) ** -0.5)

    me = lax.axis_index('tp')
    core = lax.rem(me, 2)
    chip = me // 2
    other = 1 - core
    rchip = lax.rem(chip + 1, nchip)
    lchip = lax.rem(chip + nchip - 1, nchip)
    ochip = lax.rem(chip + 2, nchip)
    mate = 2 * chip + other
    right = 2 * rchip + core
    left = 2 * lchip + core
    opp = 2 * ochip + core

    barrier = pltpu.get_barrier_semaphore()
    for peer in (mate, right, left):
        pl.semaphore_signal(barrier, inc=1, device_id={'tp': peer}, device_id_type=MESH)

    def x_copy():
        return pltpu.make_async_copy(x_hbm.at[me], xb, x_sem)

    def dq_copy(layer, i, slot):
        off = pl.multiple_of(i * kc, 128)
        return pltpu.make_async_copy(wdq.at[layer, pl.ds(off, kc), :], dq_buf.at[slot], dq_sem.at[slot])

    def kv_copy(layer, i, slot):
        off = pl.multiple_of(i * kc, 128)
        return pltpu.make_async_copy(wkv.at[layer, :, pl.ds(off, kc)], kv_buf.at[slot], kv_sem.at[slot])

    weights = [(wuq, uq_buf), (wuk, uk_buf), (wuv, uv_buf), (wo, wo_buf), (wg, wg_buf), (wu, wu_buf), (wd, wd_buf)]

    def w_copy(layer, idx):
        src, dst = weights[idx]
        return pltpu.make_async_copy(src.at[layer], dst, w_sem.at[idx])

    def ckv_copy(layer, g, slot):
        return pltpu.make_async_copy(ckv_hbm.at[layer, pl.ds(g * seqs, seqs)], ckv_buf.at[slot], c_sem.at[0, slot])

    def kpe_copy(layer, g, slot):
        return pltpu.make_async_copy(kpe_hbm.at[layer, pl.ds(g * seqs, seqs)], kpe_buf.at[slot], c_sem.at[1, slot])

    def start_dq(layer):
        for s in range(slots):
            dq_copy(layer, s, s).start()
            kv_copy(layer, s, s).start()

    def start_cache(layer):
        for s in range(2):
            ckv_copy(layer, s, s).start()
            kpe_copy(layer, s, s).start()

    def remote(src, dst, sems, recvs, j, kind, dev):
        return pltpu.make_async_remote_copy(src_ref=src, dst_ref=dst, send_sem=sems.at[j, kind],
                                            recv_sem=recvs.at[j, kind], device_id={'tp': dev}, device_id_type=MESH)

    def ag_desc(buf, j, spec, kind, blk, dev):
        off, half_a, width = spec
        lo, size = off, width
        if kind in (3, 7):
            size = half_a
        elif kind in (4, 8):
            lo, size = off + half_a, width - half_a
        ref = buf.at[blk, :, pl.ds(lo, size)]
        return remote(ref, ref, ag_send, ag_recv, j, kind, dev)

    mleft = 2 * lchip + other
    mright = 2 * rchip + other
    mopp = 2 * ochip + other
    ag_out = [(me, mate), (me, right), (me, left), (left, right), (right, left), (left, mate), (right, mate), (opp, mate), (opp, mate)]
    ag_in = [mate, left, right, opp, opp, mleft, mright, mopp, mopp]

    def ag_start(buf, j, spec, kind):
        ag_desc(buf, j, spec, kind, *ag_out[kind]).start()

    def ag_wait(buf, j, spec, kind):
        ag_desc(buf, j, spec, kind, ag_in[kind], mate).wait_recv()

    def all_gather(buf, specs, consume):
        n = len(specs)
        for j in range(n):
            for kind in (1, 2, 0):
                ag_start(buf, j, specs[j], kind)

        def forward(j):
            ag_wait(buf, j, specs[j], 1)
            ag_start(buf, j, specs[j], 3)
            ag_start(buf, j, specs[j], 5)
            ag_wait(buf, j, specs[j], 2)
            ag_start(buf, j, specs[j], 4)
            ag_start(buf, j, specs[j], 6)

        def finish(j):
            ag_wait(buf, j, specs[j], 3)
            ag_start(buf, j, specs[j], 7)
            ag_wait(buf, j, specs[j], 4)
            ag_start(buf, j, specs[j], 8)
            for kind in (0, 5, 6, 7, 8):
                ag_wait(buf, j, specs[j], kind)
            consume(j)

        forward(0)
        for j in range(1, n):
            forward(j)
            finish(j - 1)
        finish(n - 1)
        for j in range(n):
            for kind in range(9):
                ag_desc(buf, j, specs[j], kind, *ag_out[kind]).wait_send()

    def rs_desc(j, kind):
        o = j * cw
        ca, cb = pl.ds(o, ch), pl.ds(o + ch, ch)
        hj = pl.ds(j * ch, ch)
        full = pl.ds(o, cw)
        src, dst, dev = [
            lambda: (part.at[:, other, :, full], d2d.at[:, :, full], mate),
            lambda: (psum.at[ochip, :, ca], rel.at[0, :, hj], right),
            lambda: (psum.at[ochip, :, cb], rel.at[1, :, hj], left),
            lambda: (psum.at[rchip, :, cb], fin.at[0, :, cb], right),
            lambda: (psum.at[lchip, :, ca], fin.at[1, :, ca], left),
            lambda: (cmb.at[0, :, hj], fin.at[0, :, ca], right),
            lambda: (cmb.at[1, :, hj], fin.at[1, :, cb], left),
        ][kind]()
        return remote(src, dst, rs_send, rs_recv, j, kind, dev)

    def reduce_scatter(product):
        def mm(j):
            val = product(j)
            part[:, :, :, pl.ds(j * cw, cw)] = val.reshape(nchip, 2, rows, cw).astype(BF16)
            rs_desc(j, 0).start()

        def pair(j):
            rs_desc(j, 0).wait_recv()
            cols = pl.ds(j * cw, cw)
            for cc in range(nchip):
                psum[cc, :, cols] = (part[cc, core, :, cols].astype(F32) + d2d[cc, :, cols].astype(F32)).astype(BF16)
            for kind in (1, 2, 3, 4):
                rs_desc(j, kind).start()

        def combine(j):
            o = j * cw
            hj = pl.ds(j * ch, ch)
            rs_desc(j, 1).wait_recv()
            cmb[0, :, hj] = (psum[rchip, :, pl.ds(o, ch)].astype(F32) + rel[0, :, hj].astype(F32)).astype(BF16)
            rs_desc(j, 5).start()
            rs_desc(j, 2).wait_recv()
            cmb[1, :, hj] = (psum[lchip, :, pl.ds(o + ch, ch)].astype(F32) + rel[1, :, hj].astype(F32)).astype(BF16)
            rs_desc(j, 6).start()

        def final(j):
            for kind in (3, 4, 5, 6):
                rs_desc(j, kind).wait_recv()
            cols = pl.ds(j * cw, cw)
            total = psum[chip, :, cols].astype(F32) + fin[0, :, cols].astype(F32) + fin[1, :, cols].astype(F32)
            xb[:, cols] = (xb[:, cols].astype(F32) + total).astype(BF16)

        for j in range(chunks + 2):
            if j < chunks:
                mm(j)
            if 0 <= j - 1 < chunks:
                pair(j - 1)
            if 0 <= j - 2 < chunks:
                combine(j - 2)
        return final

    def rs_drain(final):
        for j in range(chunks):
            final(j)
        for j in range(chunks):
            for kind in range(7):
                rs_desc(j, kind).wait_send()

    b_specs = [(j * cw, ch, cw) for j in range(chunks)]
    qw = q_all.shape[2]
    q_specs = [(0, (qw // 256 + 1) * 128 if (qw // 128) % 2 else qw // 2, qw)]

    def gain_row(ref, layer):
        vals = ref[...].astype(F32)
        row = vals[0:1]
        for i in range(1, layers):
            row = jnp.where(layer == i, vals[i:i + 1], row)
        return row

    x_copy().start()
    start_dq(0)
    pl.semaphore_wait(barrier, 3)
    x_copy().wait()

    def layer_body(layer, carry):
        more = layer + 1 < layers
        a_buf[...] = rms(xb[...].astype(F32), gain_row(ag_ref, layer)).astype(BF16)
        acc_q[...] = jnp.zeros_like(acc_q)
        acc_kv[...] = jnp.zeros_like(acc_kv)

        def dq_step(i, c):
            slot = lax.rem(i, slots)
            dq_copy(layer, i, slot).wait()
            kv_copy(layer, i, slot).wait()
            a_c = a_buf[:, pl.ds(pl.multiple_of(i * kc, 128), kc)]
            acc_q[...] += dot_nn(a_c, dq_buf[slot])
            acc_kv[...] += dot_nt(kv_buf[slot], a_c)

            @pl.when(i + slots < n_dq)
            def _():
                dq_copy(layer, i + slots, slot).start()
                kv_copy(layer, i + slots, slot).start()
            return c

        lax.fori_loop(0, n_dq, dq_step, 0)

        @pl.when(layer == 0)
        def _():
            for idx in (0, 1, 2):
                w_copy(layer, idx).start()
            start_cache(layer)
            for idx in (3, 4, 5, 6):
                w_copy(layer, idx).start()

        q_all[me, :, pl.ds(0, lora)] = rms(acc_q[...], gain_row(qg_ref, layer)).astype(BF16)
        kv = jnp.transpose(acc_kv[...])
        q_all[me, :, pl.ds(lora, latent)] = rms(kv[:, :latent], gain_row(kg_ref, layer)).astype(BF16)
        row0 = pl.multiple_of(me * rows, rows)
        kr = kv[:, latent:latent + rope]
        kr = jnp.concatenate([kr, kr], axis=1)
        kr = kr * cos_ref[pl.ds(row0, rows), 0:2 * rope] + swap_halves(kr, rope // 2) * sin_ref[pl.ds(row0, rows), 0:2 * rope]
        lane = lax.broadcasted_iota(jnp.int32, kr.shape, 1)
        q_all[me, :, pl.ds(lora + latent, 2 * rope)] = jnp.where(lane < rope, kr, 0.0).astype(BF16)

        def nothing(j):
            return None

        all_gather(q_all, q_specs, nothing)

        out_c = pltpu.make_async_copy(q_all.at[:, :, pl.ds(lora, latent)], ckv_out.at[layer], out_sem.at[0])
        out_k = pltpu.make_async_copy(q_all.at[:, :, pl.ds(lora + latent, 2 * rope)], kpe_out.at[layer], out_sem.at[1])
        out_c.start()
        out_k.start()

        w_copy(layer, 0).wait()
        c_q = q_all[:, :, pl.ds(0, lora)].reshape(batch, lora)
        per = nope + rope
        w_n = jnp.concatenate([uq_buf[pl.ds(h * per, nope), :] for h in range(heads)], axis=0)
        w_r = jnp.concatenate([uq_buf[pl.ds(h * per + nope, rope), :] for h in range(heads)], axis=0)
        q_n = dot_nt(c_q, w_n).astype(BF16)
        q_r = dot_nt(c_q, w_r)
        q_r = q_r * cos_ref[...] + swap_halves(q_r, rope // 2) * sin_ref[...]
        lane2 = lax.broadcasted_iota(jnp.int32, (batch, 2 * rope), 1)
        for pair_i in range(heads // 2):
            duo = q_r[:, pair_i * 2 * rope:(pair_i + 1) * 2 * rope]
            swp = pltpu.roll(duo, rope, 1)
            r_buf[2 * pair_i] = jnp.where(lane2 < rope, duo, swp).astype(BF16)
            r_buf[2 * pair_i + 1] = jnp.where(lane2 < rope, swp, duo).astype(BF16)
        w_copy(layer, 1).wait()
        wf[...] = uk_buf[...].astype(F32)
        for h in range(heads):
            wk_h = wf[pl.ds(h, latent, stride=heads), :].astype(BF16)
            u_buf[h] = dot_nt(q_n[:, h * nope:(h + 1) * nope], wk_h).astype(BF16)

        @pl.when(more)
        def _():
            w_copy(layer + 1, 0).start()
            w_copy(layer + 1, 1).start()

        m_rows = heads * seqs

        def att_step(g, c):
            slot = lax.rem(g, 2)
            ckv_copy(layer, g, slot).wait()
            kpe_copy(layer, g, slot).wait()
            r0 = pl.multiple_of(g * seqs, seqs)
            cache = ckv_buf[slot].reshape(seqs * keys, latent)
            u_g = u_buf[:, pl.ds(r0, seqs), :].reshape(m_rows, latent)
            r_g = r_buf[:, pl.ds(r0, seqs), :].reshape(m_rows, 2 * rope).astype(F32)
            u_2 = jnp.concatenate([u_g, u_g], axis=0)
            s_t = dot_nt(cache, u_2)
            lane_t = lax.broadcasted_iota(jnp.int32, (keys, 2 * m_rows), 1) % seqs
            sel = s_t[0:keys]
            for b in range(1, seqs):
                sel = jnp.where(lane_t == b, s_t[b * keys:(b + 1) * keys], sel)
            s_n = jnp.transpose(sel)[0:m_rows]
            row_b = lax.broadcasted_iota(jnp.int32, (m_rows, keys), 0) % seqs
            lane_k = lax.broadcasted_iota(jnp.int32, (m_rows, keys), 1)
            row_r = lax.broadcasted_iota(jnp.int32, (m_rows, 2 * rope), 0) % seqs
            lane_r = lax.broadcasted_iota(jnp.int32, (m_rows, 2 * rope), 1) // rope
            q_blk = jnp.concatenate(
                [jnp.where(row_r == 2 * b + lane_r, r_g, 0.0).astype(BF16) for b in range(seqs // 2)], axis=1)
            s_r = dot_nn(q_blk, kpe_buf[slot].reshape(seqs * rope, keys))
            cn = tile_rows(q_all[g, :, pl.ds(lora, latent)].astype(F32), heads)
            kn = tile_rows(q_all[g, :, pl.ds(lora + latent, 2 * rope)].astype(F32), heads)
            fresh = jnp.sum(u_g.astype(F32) * cn, axis=-1, keepdims=True) + jnp.sum(r_g * kn, axis=-1, keepdims=True)
            pos = tile_rows(pos_ref[pl.ds(r0, seqs), :], heads)
            at_pos = lane_k == pos
            s = jnp.where(at_pos, fresh, s_n + s_r) * scale
            s = jnp.where(lane_k <= pos, s, NEG_INF)
            e = jnp.exp(s - jnp.max(s, axis=-1, keepdims=True))
            prob = (e / jnp.sum(e, axis=-1, keepdims=True)).astype(BF16).astype(F32)
            p_new = jnp.sum(jnp.where(at_pos, prob, 0.0), axis=-1, keepdims=True)
            p_old = jnp.where(at_pos, 0.0, prob)
            p_blk = jnp.concatenate([jnp.where(row_b == b, p_old, 0.0).astype(BF16) for b in range(seqs)], axis=1)
            ctx = dot_nn(p_blk, cache) + p_new * cn
            ctx_buf[:, pl.ds(r0, seqs), :] = ctx.astype(BF16).reshape(heads, seqs, latent)

            @pl.when(g + 2 < batch // seqs)
            def _():
                ckv_copy(layer, g + 2, slot).start()
                kpe_copy(layer, g + 2, slot).start()
            return c

        lax.fori_loop(0, batch // seqs, att_step, 0)

        w_copy(layer, 2).wait()
        wf[...] = uv_buf[...].astype(F32)
        for h in range(heads):
            wv_h = wf[pl.ds(h, latent, stride=heads), :].astype(BF16)
            o_buf[:, h * nope:(h + 1) * nope] = dot_nn(ctx_buf[h], wv_h).astype(BF16)

        @pl.when(more)
        def _():
            w_copy(layer + 1, 2).start()

        w_copy(layer, 3).wait()
        out_c.wait()
        out_k.wait()

        final = reduce_scatter(lambda j: dot_nn(o_buf[...], wo_buf[:, pl.ds(j * cw, cw)]))

        @pl.when(more)
        def _():
            start_dq(layer + 1)
            start_cache(layer + 1)
            w_copy(layer + 1, 3).start()

        rs_drain(final)

        b_all[me] = rms(xb[...].astype(F32), gain_row(mg_ref, layer)).astype(BF16)
        w_copy(layer, 4).wait()
        w_copy(layer, 5).wait()

        def gate_up(j):
            cols = pl.ds(j * cw, cw)
            b_c = b_all[:, :, cols].reshape(batch, cw)
            g_v = dot_nt(wg_buf[:, cols], b_c)
            u_v = dot_nt(wu_buf[:, cols], b_c)
            if j == 0:
                gate_acc[...] = g_v
                up_acc[...] = u_v
            else:
                gate_acc[...] += g_v
                up_acc[...] += u_v

        all_gather(b_all, b_specs, gate_up)
        gate = gate_acc[...]
        act_buf[...] = jnp.transpose(gate * lax.logistic(gate) * up_acc[...]).astype(BF16)
        w_copy(layer, 6).wait()

        @pl.when(more)
        def _():
            w_copy(layer + 1, 4).start()
            w_copy(layer + 1, 5).start()

        final2 = reduce_scatter(lambda j: dot_nn(act_buf[...], wd_buf[:, pl.ds(j * cw, cw)]))

        @pl.when(more)
        def _():
            w_copy(layer + 1, 6).start()

        rs_drain(final2)
        return carry

    lax.fori_loop(0, layers, layer_body, 0)

    b_all[me] = xb[...]

    def put(j):
        cols = pl.ds(j * cw, cw)
        pltpu.make_async_copy(b_all.at[:, :, cols], x_out.at[:, :, cols], out_sem.at[j]).start()

    all_gather(b_all, b_specs, put)
    for j in range(chunks):
        cols = pl.ds(j * cw, cw)
        pltpu.make_async_copy(b_all.at[:, :, cols], x_out.at[:, :, cols], out_sem.at[j]).wait()


def solution(mesh):
    tp = mesh.shape['tp']
    cache_spec = P(None, 'dp', None, None)
    head_spec = P(None, None, 'tp', None)
    weight_specs = (P(), P(), P(), P(), P(), head_spec, head_spec, head_spec, P(None, 'tp', None, None), P(), P(None, None, 'tp'), P(None, None, 'tp'), P(None, 'tp', None))
    in_specs = (P('dp', None), P('dp'), cache_spec, cache_spec) + weight_specs
    out_specs = (P('dp', None), P(None, 'dp', None), P(None, 'dp', None))

    def device_body(x_in, pos_ids, ckv_cache, kpe_cache, attn_gain, w_dq, q_gain, w_dkv, kv_gain, w_uq, w_uk, w_uv, w_o,
                    mlp_gain, w_gate, w_up, w_down):
        batch, model = x_in.shape
        layers, _, keys, latent = ckv_cache.shape
        rope = kpe_cache.shape[-1]
        lora = w_dq.shape[-1]
        heads, per = w_uq.shape[2:]
        nope = w_uk.shape[-1]
        ffn = w_gate.shape[-1]
        rows = batch // tp
        kc, slots, chunks, seqs = 512, 4, 4, rows
        half = rope // 2

        inv_freq = jnp.exp(jnp.arange(half, dtype=F32) * (-2.0 * math.log(ROPE_BASE) / rope))
        angles = pos_ids.astype(F32)[:, None] * inv_freq
        cos, sin = jnp.cos(angles), jnp.sin(angles)
        cos_t = jnp.tile(jnp.concatenate([cos, cos], axis=1), (1, heads))
        sin_t = jnp.tile(jnp.concatenate([-sin, sin], axis=1), (1, heads))
        pos_t = jnp.broadcast_to(pos_ids[:, None], (batch, keys))

        vm = pl.BlockSpec(memory_space=pltpu.VMEM)
        hb = pl.BlockSpec(memory_space=pl.ANY)
        dma = pltpu.SemaphoreType.DMA
        qw = lora + latent + 2 * rope
        ch = model // chunks // 2
        scratch = [
            pltpu.VMEM((rows, model), BF16),
            pltpu.VMEM((rows, model), BF16),
            pltpu.VMEM((tp, rows, model), BF16),
            pltpu.VMEM((tp, rows, qw), BF16),
            pltpu.VMEM((rows, lora), F32),
            pltpu.VMEM((latent + rope, rows), F32),
            pltpu.VMEM((heads, batch, latent), BF16),
            pltpu.VMEM((heads, batch, 2 * rope), BF16),
            pltpu.VMEM((heads, batch, latent), BF16),
            pltpu.VMEM((batch, heads * nope), BF16),
            pltpu.VMEM((latent * heads, nope), F32),
            pltpu.VMEM((ffn, batch), F32),
            pltpu.VMEM((ffn, batch), F32),
            pltpu.VMEM((batch, ffn), BF16),
            pltpu.VMEM((tp // 2, 2, rows, model), BF16),
            pltpu.VMEM((tp // 2, rows, model), BF16),
            pltpu.VMEM((tp // 2, rows, model), BF16),
            pltpu.VMEM((2, rows, model // 2), BF16),
            pltpu.VMEM((2, rows, model // 2), BF16),
            pltpu.VMEM((2, rows, model), BF16),
            pltpu.VMEM((slots, kc, lora), BF16),
            pltpu.VMEM((slots, latent + rope, kc), BF16),
            pltpu.VMEM((heads * per, lora), BF16),
            pltpu.VMEM((latent * heads, nope), BF16),
            pltpu.VMEM((latent * heads, nope), BF16),
            pltpu.VMEM((heads * nope, model), BF16),
            pltpu.VMEM((ffn, model), BF16),
            pltpu.VMEM((ffn, model), BF16),
            pltpu.VMEM((ffn, model), BF16),
            pltpu.VMEM((2, seqs, keys, latent), BF16),
            pltpu.VMEM((2, seqs, rope, keys), BF16),
            dma(()), dma((slots,)), dma((slots,)), dma((7,)), dma((2, 2)), dma((max(chunks, 2),)),
            dma((chunks, 9)), dma((chunks, 9)), dma((chunks, 7)), dma((chunks, 7)),
        ]
        cfg = dict(tp=tp, layers=layers, heads=heads, kc=kc, slots=slots, chunks=chunks, seqs=seqs)
        call = pl.pallas_call(
            functools.partial(step_kernel, cfg),
            out_shape=(jax.ShapeDtypeStruct((tp, rows, model), BF16),
                       jax.ShapeDtypeStruct((layers, tp, rows, latent), BF16),
                       jax.ShapeDtypeStruct((layers, tp, rows, 2 * rope), BF16)),
            in_specs=[hb, vm, vm, vm, vm, vm, vm, vm] + [hb] * 11,
            out_specs=(hb, hb, hb),
            scratch_shapes=scratch,
            compiler_params=pltpu.CompilerParams(collective_id=0, has_side_effects=True, vmem_limit_bytes=67043328),
            name='decode_step',
        )
        x_o, c_o, k_o = call(
            x_in.reshape(tp, rows, model), cos_t, sin_t, pos_t, attn_gain, mlp_gain, q_gain, kv_gain,
            w_dq, w_dkv.transpose(0, 2, 1), w_uq.transpose(0, 2, 3, 1).reshape(layers, heads * per, lora),
            w_uk.reshape(layers, latent * heads, nope), w_uv.reshape(layers, latent * heads, nope),
            w_o.reshape(layers, heads * nope, model),
            w_gate.transpose(0, 2, 1), w_up.transpose(0, 2, 1), w_down,
            ckv_cache, kpe_cache.transpose(0, 1, 3, 2))
        return (x_o.reshape(batch, model), c_o.reshape(layers, batch, latent),
                k_o.reshape(layers, batch, 2 * rope)[..., :rope])

    return jax.shard_map(device_body, mesh=mesh, in_specs=in_specs, out_specs=out_specs, check_vma=False)
```

```python
import math
import functools
import jax
import jax.numpy as jnp
from jax import lax
from jax.experimental import pallas as pl
from jax.experimental.pallas import tpu as pltpu
from jax.sharding import PartitionSpec as P

NORM_EPS = 1e-6
ROPE_BASE = 10000.0
F32 = jnp.float32
BF16 = jnp.bfloat16
MESH = pl.DeviceIdType.MESH
NEG_INF = float('-inf')


def rms(values, gain):
    inv = lax.rsqrt(jnp.mean(values * values, axis=-1, keepdims=True) + NORM_EPS)
    return values * inv * gain


def dot_nt(lhs, rhs):
    return lax.dot_general(lhs, rhs, (((1,), (1,)), ((), ())), preferred_element_type=F32)


def dot_nn(lhs, rhs):
    return jnp.dot(lhs, rhs, preferred_element_type=F32)


def swap_halves(values, half):
    width = values.shape[-1]
    lane = lax.broadcasted_iota(jnp.int32, values.shape, 1)
    up = pltpu.roll(values, half, 1)
    down = pltpu.roll(values, width - half, 1)
    return jnp.where(lane % (2 * half) < half, down, up)


def tile_rows(values, count):
    return jnp.concatenate([values] * count, axis=0)


def step_kernel(cfg, x_hbm, pos_hbm, ag_hbm, mg_hbm, qg_hbm, kg_hbm,
                wdq, wkv, wuq, wuk, wuv, wo, wg, wu, wd, ckv_hbm, kpe_hbm,
                x_out, ckv_out, kpe_out,
                pos_row, ag_ref, mg_ref, qg_ref, kg_ref, cos_ref, sin_ref, pos_ref,
                xb, a_buf, a_pair, acc_in, b_all, q_all, acc_q, u_buf, r_buf, ctx_buf, o_buf, wf,
                gu_acc, act_buf,
                part, d2d, psum, rel, cmb, fin,
                dq_buf, kv_buf, uq_buf, uk_buf, uv_buf, wo_buf, wgu_buf, wd_buf, ckv_buf, kpe_buf,
                x_sem, s_sem, px_sem, dq_sem, kv_sem, w_sem, c_sem, out_sem,
                ag_send, ag_recv, rs_send, rs_recv):
    tp_size, layers, heads, kc, slots, chunks, seqs = (
        cfg['tp'], cfg['layers'], cfg['heads'], cfg['kc'], cfg['slots'], cfg['chunks'], cfg['seqs'])
    nchip = tp_size // 2
    model = xb.shape[1]
    rows = xb.shape[0]
    lora = uq_buf.shape[1]
    latent = ckv_buf.shape[-1]
    rope = kpe_buf.shape[2]
    nope = uk_buf.shape[1]
    keys = ckv_buf.shape[2]
    batch = rows * tp_size
    ffn = wd_buf.shape[0]
    half_k = model // 2
    n_dq = half_k // kc
    cw = model // chunks
    ch = cw // 2
    scale = float((nope + rope) ** -0.5)

    me = lax.axis_index('tp')
    core = lax.rem(me, 2)
    chip = me // 2
    other = 1 - core
    rchip = lax.rem(chip + 1, nchip)
    lchip = lax.rem(chip + nchip - 1, nchip)
    ochip = lax.rem(chip + 2, nchip)
    mate = 2 * chip + other
    right = 2 * rchip + core
    left = 2 * lchip + core
    opp = 2 * ochip + core

    barrier = pltpu.get_barrier_semaphore()
    for peer in (mate, right, left, opp):
        pl.semaphore_signal(barrier, inc=1, device_id={'tp': peer}, device_id_type=MESH)

    def x_copy():
        return pltpu.make_async_copy(x_hbm.at[me], xb, x_sem)

    def dq_copy(layer, i, slot):
        off = pl.multiple_of(core * half_k + i * kc, 128)
        return pltpu.make_async_copy(wdq.at[layer, pl.ds(off, kc), :], dq_buf.at[slot], dq_sem.at[slot])

    def kv_copy(layer, i, slot):
        off = pl.multiple_of(core * half_k + i * kc, 128)
        return pltpu.make_async_copy(wkv.at[layer, :, pl.ds(off, kc)], kv_buf.at[slot], kv_sem.at[slot])

    weights = [(wuq, uq_buf), (wuk, uk_buf), (wuv, uv_buf), (wo, wo_buf), (wg, wgu_buf.at[0:ffn]), (wu, wgu_buf.at[ffn:2 * ffn]), (wd, wd_buf)]

    def w_copy(layer, idx):
        src, dst = weights[idx]
        return pltpu.make_async_copy(src.at[layer], dst, w_sem.at[idx])

    def ckv_copy(layer, g, slot):
        return pltpu.make_async_copy(ckv_hbm.at[layer, pl.ds(g * seqs, seqs)], ckv_buf.at[slot], c_sem.at[0, slot])

    def kpe_copy(layer, g, slot):
        return pltpu.make_async_copy(kpe_hbm.at[layer, pl.ds(g * seqs, seqs)], kpe_buf.at[slot], c_sem.at[1, slot])

    def start_dq(layer):
        for s in range(slots):
            dq_copy(layer, s, s).start()
            kv_copy(layer, s, s).start()

    def start_cache(layer):
        for s in range(2):
            ckv_copy(layer, s, s).start()
            kpe_copy(layer, s, s).start()

    def remote(src, dst, sems, recvs, j, kind, dev):
        return pltpu.make_async_remote_copy(src_ref=src, dst_ref=dst, send_sem=sems.at[j, kind],
                                            recv_sem=recvs.at[j, kind], device_id={'tp': dev}, device_id_type=MESH)

    def ag_desc(buf, j, spec, kind, blk, dev):
        off, half_a, width = spec
        lo, size = off, width
        if kind in (3, 7):
            size = half_a
        elif kind in (4, 8):
            lo, size = off + half_a, width - half_a
        ref = buf.at[blk, :, pl.ds(lo, size)]
        return remote(ref, ref, ag_send, ag_recv, j, kind, dev)

    mleft = 2 * lchip + other
    mright = 2 * rchip + other
    mopp = 2 * ochip + other
    ag_out = [(me, mate), (me, right), (me, left), (left, right), (right, left), (left, mate), (right, mate), (opp, mate), (opp, mate)]
    ag_in = [mate, left, right, opp, opp, mleft, mright, mopp, mopp]

    def ag_start(buf, j, spec, kind):
        ag_desc(buf, j, spec, kind, *ag_out[kind]).start()

    def ag_wait(buf, j, spec, kind):
        ag_desc(buf, j, spec, kind, ag_in[kind], mate).wait_recv()

    def all_gather(buf, specs, consume):
        n = len(specs)
        for j in range(n):
            for kind in (1, 2, 0):
                ag_start(buf, j, specs[j], kind)

        def forward(j):
            ag_wait(buf, j, specs[j], 1)
            ag_start(buf, j, specs[j], 3)
            ag_start(buf, j, specs[j], 5)
            ag_wait(buf, j, specs[j], 2)
            ag_start(buf, j, specs[j], 4)
            ag_start(buf, j, specs[j], 6)

        def finish(j):
            with jax.named_scope('wait_opp'):
                ag_wait(buf, j, specs[j], 3)
                ag_start(buf, j, specs[j], 7)
                ag_wait(buf, j, specs[j], 4)
                ag_start(buf, j, specs[j], 8)
            with jax.named_scope('wait_near'):
                for kind in (0, 5, 6):
                    ag_wait(buf, j, specs[j], kind)
            with jax.named_scope('wait_far'):
                for kind in (7, 8):
                    ag_wait(buf, j, specs[j], kind)
            with jax.named_scope('consume'):
                consume(j)

        forward(0)
        for j in range(1, n):
            forward(j)
            finish(j - 1)
        finish(n - 1)
        for j in range(n):
            for kind in range(9):
                ag_desc(buf, j, specs[j], kind, *ag_out[kind]).wait_send()

    def rs_desc(j, kind):
        o = j * cw
        ca, cb = pl.ds(o, ch), pl.ds(o + ch, ch)
        hj = pl.ds(j * ch, ch)
        full = pl.ds(o, cw)
        src, dst, dev = [
            lambda: (part.at[:, other, :, full], d2d.at[:, :, full], mate),
            lambda: (psum.at[ochip, :, ca], rel.at[0, :, hj], right),
            lambda: (psum.at[ochip, :, cb], rel.at[1, :, hj], left),
            lambda: (psum.at[rchip, :, cb], fin.at[0, :, cb], right),
            lambda: (psum.at[lchip, :, ca], fin.at[1, :, ca], left),
            lambda: (cmb.at[0, :, hj], fin.at[0, :, ca], right),
            lambda: (cmb.at[1, :, hj], fin.at[1, :, cb], left),
        ][kind]()
        return remote(src, dst, rs_send, rs_recv, j, kind, dev)

    def reduce_scatter(product):
        def mm(j):
            val = product(j)
            part[:, :, :, pl.ds(j * cw, cw)] = val.reshape(nchip, 2, rows, cw).astype(BF16)
            rs_desc(j, 0).start()

        def pair(j):
            rs_desc(j, 0).wait_recv()
            cols = pl.ds(j * cw, cw)
            psum[ochip, :, cols] = (part[ochip, core, :, cols].astype(F32) + d2d[ochip, :, cols].astype(F32)).astype(BF16)
            rs_desc(j, 1).start()
            rs_desc(j, 2).start()
            for cc in (rchip, lchip, chip):
                psum[cc, :, cols] = (part[cc, core, :, cols].astype(F32) + d2d[cc, :, cols].astype(F32)).astype(BF16)

        def combine(j):
            o = j * cw
            hj = pl.ds(j * ch, ch)
            rs_desc(j, 1).wait_recv()
            cmb[0, :, hj] = (psum[rchip, :, pl.ds(o, ch)].astype(F32) + rel[0, :, hj].astype(F32)).astype(BF16)
            rs_desc(j, 5).start()
            rs_desc(j, 2).wait_recv()
            cmb[1, :, hj] = (psum[lchip, :, pl.ds(o + ch, ch)].astype(F32) + rel[1, :, hj].astype(F32)).astype(BF16)
            rs_desc(j, 6).start()

        def final(j):
            for kind in (3, 4, 5, 6):
                rs_desc(j, kind).wait_recv()
            cols = pl.ds(j * cw, cw)
            total = psum[chip, :, cols].astype(F32) + fin[0, :, cols].astype(F32) + fin[1, :, cols].astype(F32)
            xb[:, cols] = (xb[:, cols].astype(F32) + total).astype(BF16)

        for j in range(chunks + 1):
            if j < chunks:
                mm(j)
            if j > 0:
                pair(j - 1)
        for j in range(chunks):
            rs_desc(j, 3).start()
            rs_desc(j, 4).start()
        for j in range(chunks):
            combine(j)
        return final

    def rs_drain(final):
        for j in range(chunks):
            final(j)
        for j in range(chunks):
            for kind in range(7):
                rs_desc(j, kind).wait_send()

    b_specs = [(j * cw, ch, cw) for j in range(chunks)]
    qw = q_all.shape[2]
    q_specs = [(0, (qw // 256 + 1) * 128 if (qw // 128) % 2 else qw // 2, qw)]

    def gain_row(ref, layer):
        vals = ref[...].astype(F32)
        row = vals[0:1]
        for i in range(1, layers):
            row = jnp.where(layer == i, vals[i:i + 1], row)
        return row

    small = [(pos_hbm, pos_row), (ag_hbm, ag_ref), (mg_hbm, mg_ref), (qg_hbm, qg_ref), (kg_hbm, kg_ref)]
    x_copy().start()
    for i, (src, dst) in enumerate(small):
        pltpu.make_async_copy(src, dst, s_sem.at[i]).start()
    start_dq(0)
    for i, (src, dst) in enumerate(small):
        pltpu.make_async_copy(src, dst, s_sem.at[i]).wait()
    pos_f = jnp.transpose(jnp.broadcast_to(pos_row[...].astype(F32), (batch, batch)))
    pos_ref[...] = pos_f.astype(jnp.int32)
    lane_f = lax.broadcasted_iota(jnp.int32, (batch, batch), 1) % (rope // 2)
    angles = pos_f * jnp.exp(lane_f.astype(F32) * (-2.0 * math.log(ROPE_BASE) / rope))
    cos_v, sin_v = jnp.cos(angles), jnp.sin(angles)
    lane_s = lax.broadcasted_iota(jnp.int32, (batch, batch), 1) % rope
    sin_v = jnp.where(lane_s < rope // 2, -sin_v, sin_v)
    for i in range(heads * rope // batch):
        cos_ref[:, i * batch:(i + 1) * batch] = cos_v
        sin_ref[:, i * batch:(i + 1) * batch] = sin_v
    x_copy().wait()

    def pair_copy(src, dst, i):
        return pltpu.make_async_remote_copy(src_ref=src, dst_ref=dst, send_sem=px_sem.at[0, i], recv_sem=px_sem.at[1, i],
                                            device_id={'tp': mate}, device_id_type=MESH)

    def layer_body(layer, carry):
        more = layer + 1 < layers
        a_buf[...] = rms(xb[...].astype(F32), gain_row(ag_ref, layer)).astype(BF16)

        @pl.when(layer == 0)
        def _():
            pl.semaphore_wait(barrier, 4)

        swap = pair_copy(a_buf.at[:, pl.ds(pl.multiple_of(other * half_k, 128), half_k)], a_pair.at[1], 0)
        swap.start()
        a_pair[0] = a_buf[:, pl.ds(pl.multiple_of(core * half_k, 128), half_k)]
        acc_q[...] = jnp.zeros_like(acc_q)
        swap.wait_recv()

        def dq_step(i, c):
            slot = lax.rem(i, slots)
            dq_copy(layer, i, slot).wait()
            kv_copy(layer, i, slot).wait()
            a_c = a_pair[:, :, pl.ds(pl.multiple_of(i * kc, 128), kc)].reshape(2 * rows, kc)
            acc_q[:, :, 0:lora] += dot_nn(a_c, dq_buf[slot]).reshape(2, rows, lora)
            acc_q[:, :, lora:lora + latent + rope] += dot_nt(a_c, kv_buf[slot]).reshape(2, rows, latent + rope)

            @pl.when(i + slots < n_dq)
            def _():
                dq_copy(layer, i + slots, slot).start()
                kv_copy(layer, i + slots, slot).start()
            return c

        lax.fori_loop(0, n_dq, dq_step, 0)

        @pl.when(layer == 0)
        def _():
            for idx in (0, 1, 2):
                w_copy(layer, idx).start()
            start_cache(layer)
            for idx in (3, 4, 5, 6):
                w_copy(layer, idx).start()

        back = pair_copy(acc_q.at[1], acc_in, 1)
        back.start()
        back.wait_recv()
        lat = acc_q[0] + acc_in[...]
        q_all[me, :, pl.ds(0, lora)] = rms(lat[:, :lora], gain_row(qg_ref, layer)).astype(BF16)
        kv = lat[:, lora:]
        q_all[me, :, pl.ds(lora, latent)] = rms(kv[:, :latent], gain_row(kg_ref, layer)).astype(BF16)
        row0 = pl.multiple_of(me * rows, rows)
        kr = kv[:, latent:latent + rope]
        kr = jnp.concatenate([kr, kr], axis=1)
        kr = kr * cos_ref[pl.ds(row0, rows), 0:2 * rope] + swap_halves(kr, rope // 2) * sin_ref[pl.ds(row0, rows), 0:2 * rope]
        lane = lax.broadcasted_iota(jnp.int32, kr.shape, 1)
        q_all[me, :, pl.ds(lora + latent, 2 * rope)] = jnp.where(lane < rope, kr, 0.0).astype(BF16)

        def nothing(j):
            return None

        swap.wait_send()
        back.wait_send()
        all_gather(q_all, q_specs, nothing)

        out_c = pltpu.make_async_copy(q_all.at[:, :, pl.ds(lora, latent)], ckv_out.at[layer], out_sem.at[0])
        out_k = pltpu.make_async_copy(q_all.at[:, :, pl.ds(lora + latent, 2 * rope)], kpe_out.at[layer], out_sem.at[1])
        out_c.start()
        out_k.start()

        w_copy(layer, 0).wait()
        c_q = q_all[:, :, pl.ds(0, lora)].reshape(batch, lora)
        per = nope + rope
        w_n = jnp.concatenate([uq_buf[pl.ds(h * per, nope), :] for h in range(heads)], axis=0)
        w_r = jnp.concatenate([uq_buf[pl.ds(h * per + nope, rope), :] for h in range(heads)], axis=0)
        q_n = dot_nt(c_q, w_n).astype(BF16)
        q_r = dot_nt(c_q, w_r)
        q_r = q_r * cos_ref[...] + swap_halves(q_r, rope // 2) * sin_ref[...]
        lane2 = lax.broadcasted_iota(jnp.int32, (batch, 2 * rope), 1)
        for pair_i in range(heads // 2):
            duo = q_r[:, pair_i * 2 * rope:(pair_i + 1) * 2 * rope]
            swp = pltpu.roll(duo, rope, 1)
            r_buf[2 * pair_i] = jnp.where(lane2 < rope, duo, swp).astype(BF16)
            r_buf[2 * pair_i + 1] = jnp.where(lane2 < rope, swp, duo).astype(BF16)
        w_copy(layer, 1).wait()
        wf[...] = uk_buf[...].astype(F32)
        for h in range(heads):
            wk_h = wf[pl.ds(h, latent, stride=heads), :].astype(BF16)
            u_buf[h] = dot_nt(q_n[:, h * nope:(h + 1) * nope], wk_h).astype(BF16)

        @pl.when(more)
        def _():
            w_copy(layer + 1, 0).start()
            w_copy(layer + 1, 1).start()

        m_rows = heads * seqs

        def att_step(g, c):
            slot = lax.rem(g, 2)
            ckv_copy(layer, g, slot).wait()
            kpe_copy(layer, g, slot).wait()
            r0 = pl.multiple_of(g * seqs, seqs)
            cache = ckv_buf[slot].reshape(seqs * keys, latent)
            u_g = u_buf[:, pl.ds(r0, seqs), :].reshape(m_rows, latent)
            r_g = r_buf[:, pl.ds(r0, seqs), :].reshape(m_rows, 2 * rope).astype(F32)
            row_b = lax.broadcasted_iota(jnp.int32, (m_rows, keys), 0) % seqs
            s_t = dot_nt(u_g, cache)
            s_n = s_t[:, 0:keys]
            for b in range(1, seqs):
                s_n = jnp.where(row_b == b, s_t[:, b * keys:(b + 1) * keys], s_n)
            lane_k = lax.broadcasted_iota(jnp.int32, (m_rows, keys), 1)
            row_r = lax.broadcasted_iota(jnp.int32, (m_rows, 2 * rope), 0) % seqs
            lane_r = lax.broadcasted_iota(jnp.int32, (m_rows, 2 * rope), 1) // rope
            q_blk = jnp.concatenate(
                [jnp.where(row_r == 2 * b + lane_r, r_g, 0.0).astype(BF16) for b in range(seqs // 2)], axis=1)
            s_r = dot_nn(q_blk, kpe_buf[slot].reshape(seqs * rope, keys))
            cn = tile_rows(q_all[g, :, pl.ds(lora, latent)].astype(F32), heads)
            kn = tile_rows(q_all[g, :, pl.ds(lora + latent, 2 * rope)].astype(F32), heads)
            fresh = jnp.sum(u_g.astype(F32) * cn, axis=-1, keepdims=True) + jnp.sum(r_g * kn, axis=-1, keepdims=True)
            pos = tile_rows(pos_ref[pl.ds(r0, seqs), :], heads)
            at_pos = lane_k == pos
            s = jnp.where(at_pos, fresh, s_n + s_r) * scale
            s = jnp.where(lane_k <= pos, s, NEG_INF)
            e = jnp.exp(s - jnp.max(s, axis=-1, keepdims=True))
            prob = (e / jnp.sum(e, axis=-1, keepdims=True)).astype(BF16).astype(F32)
            p_new = jnp.sum(jnp.where(at_pos, prob, 0.0), axis=-1, keepdims=True)
            p_old = jnp.where(at_pos, 0.0, prob)
            p_blk = jnp.concatenate([jnp.where(row_b == b, p_old, 0.0).astype(BF16) for b in range(seqs)], axis=1)
            ctx = dot_nn(p_blk, cache) + p_new * cn
            ctx_buf[:, pl.ds(r0, seqs), :] = ctx.astype(BF16).reshape(heads, seqs, latent)

            @pl.when(g + 2 < batch // seqs)
            def _():
                ckv_copy(layer, g + 2, slot).start()
                kpe_copy(layer, g + 2, slot).start()
            return c

        lax.fori_loop(0, batch // seqs, att_step, 0)

        w_copy(layer, 2).wait()
        wf[...] = uv_buf[...].astype(F32)
        for h in range(heads):
            wv_h = wf[pl.ds(h, latent, stride=heads), :].astype(BF16)
            o_buf[:, h * nope:(h + 1) * nope] = dot_nn(ctx_buf[h], wv_h).astype(BF16)

        @pl.when(more)
        def _():
            w_copy(layer + 1, 2).start()

        w_copy(layer, 3).wait()
        out_c.wait()
        out_k.wait()

        final = reduce_scatter(lambda j: dot_nn(o_buf[...], wo_buf[:, pl.ds(j * cw, cw)]))

        @pl.when(more)
        def _():
            start_dq(layer + 1)
            start_cache(layer + 1)
            w_copy(layer + 1, 3).start()

        rs_drain(final)

        b_all[me] = rms(xb[...].astype(F32), gain_row(mg_ref, layer)).astype(BF16)
        w_copy(layer, 4).wait()
        w_copy(layer, 5).wait()

        def gate_up(j):
            cols = pl.ds(j * cw, cw)
            b_c = b_all[:, :, cols].reshape(batch, cw)
            val = dot_nt(b_c, wgu_buf[:, cols])
            if j == 0:
                gu_acc[...] = val
            else:
                gu_acc[...] += val

        all_gather(b_all, b_specs, gate_up)
        gate = gu_acc[:, 0:ffn]
        act_buf[...] = (gate * lax.logistic(gate) * gu_acc[:, ffn:2 * ffn]).astype(BF16)
        w_copy(layer, 6).wait()

        @pl.when(more)
        def _():
            w_copy(layer + 1, 4).start()
            w_copy(layer + 1, 5).start()

        final2 = reduce_scatter(lambda j: dot_nn(act_buf[...], wd_buf[:, pl.ds(j * cw, cw)]))

        @pl.when(more)
        def _():
            w_copy(layer + 1, 6).start()

        rs_drain(final2)
        return carry

    lax.fori_loop(0, layers, layer_body, 0)

    b_all[me] = xb[...]

    def put(j):
        cols = pl.ds(j * cw, cw)
        pltpu.make_async_copy(b_all.at[:, :, cols], x_out.at[:, :, cols], out_sem.at[j]).start()

    all_gather(b_all, b_specs, put)
    for j in range(chunks):
        cols = pl.ds(j * cw, cw)
        pltpu.make_async_copy(b_all.at[:, :, cols], x_out.at[:, :, cols], out_sem.at[j]).wait()


def solution(mesh):
    tp = mesh.shape['tp']
    cache_spec = P(None, 'dp', None, None)
    head_spec = P(None, None, 'tp', None)
    weight_specs = (P(), P(), P(), P(), P(), head_spec, head_spec, head_spec, P(None, 'tp', None, None), P(), P(None, None, 'tp'), P(None, None, 'tp'), P(None, 'tp', None))
    in_specs = (P('dp', None), P('dp'), cache_spec, cache_spec) + weight_specs
    out_specs = (P('dp', None), P(None, 'dp', None), P(None, 'dp', None))

    def device_body(x_in, pos_ids, ckv_cache, kpe_cache, attn_gain, w_dq, q_gain, w_dkv, kv_gain, w_uq, w_uk, w_uv, w_o,
                    mlp_gain, w_gate, w_up, w_down):
        batch, model = x_in.shape
        layers, _, keys, latent = ckv_cache.shape
        rope = kpe_cache.shape[-1]
        lora = w_dq.shape[-1]
        heads, per = w_uq.shape[2:]
        nope = w_uk.shape[-1]
        ffn = w_gate.shape[-1]
        rows = batch // tp
        kc, slots, chunks, seqs = 512, 4, 4, rows
        hb = pl.BlockSpec(memory_space=pl.ANY)
        dma = pltpu.SemaphoreType.DMA
        qw = lora + latent + 2 * rope
        ch = model // chunks // 2
        scratch = [
            pltpu.VMEM((1, batch), jnp.int32),
            pltpu.VMEM((layers, model), BF16),
            pltpu.VMEM((layers, model), BF16),
            pltpu.VMEM((layers, lora), BF16),
            pltpu.VMEM((layers, latent), BF16),
            pltpu.VMEM((batch, heads * rope), F32),
            pltpu.VMEM((batch, heads * rope), F32),
            pltpu.VMEM((batch, keys), jnp.int32),
            pltpu.VMEM((rows, model), BF16),
            pltpu.VMEM((rows, model), BF16),
            pltpu.VMEM((2, rows, model // 2), BF16),
            pltpu.VMEM((rows, lora + latent + 2 * rope), F32),
            pltpu.VMEM((tp, rows, model), BF16),
            pltpu.VMEM((tp, rows, qw), BF16),
            pltpu.VMEM((2, rows, lora + latent + 2 * rope), F32),
            pltpu.VMEM((heads, batch, latent), BF16),
            pltpu.VMEM((heads, batch, 2 * rope), BF16),
            pltpu.VMEM((heads, batch, latent), BF16),
            pltpu.VMEM((batch, heads * nope), BF16),
            pltpu.VMEM((latent * heads, nope), F32),
            pltpu.VMEM((batch, 2 * ffn), F32),
            pltpu.VMEM((batch, ffn), BF16),
            pltpu.VMEM((tp // 2, 2, rows, model), BF16),
            pltpu.VMEM((tp // 2, rows, model), BF16),
            pltpu.VMEM((tp // 2, rows, model), BF16),
            pltpu.VMEM((2, rows, model // 2), BF16),
            pltpu.VMEM((2, rows, model // 2), BF16),
            pltpu.VMEM((2, rows, model), BF16),
            pltpu.VMEM((slots, kc, lora), BF16),
            pltpu.VMEM((slots, latent + rope, kc), BF16),
            pltpu.VMEM((heads * per, lora), BF16),
            pltpu.VMEM((latent * heads, nope), BF16),
            pltpu.VMEM((latent * heads, nope), BF16),
            pltpu.VMEM((heads * nope, model), BF16),
            pltpu.VMEM((2 * ffn, model), BF16),
            pltpu.VMEM((ffn, model), BF16),
            pltpu.VMEM((2, seqs, keys, latent), BF16),
            pltpu.VMEM((2, seqs, rope, keys), BF16),
            dma(()), dma((5,)), dma((2, 2)), dma((slots,)), dma((slots,)), dma((7,)), dma((2, 2)), dma((max(chunks, 2),)),
            dma((chunks, 9)), dma((chunks, 9)), dma((chunks, 7)), dma((chunks, 7)),
        ]
        cfg = dict(tp=tp, layers=layers, heads=heads, kc=kc, slots=slots, chunks=chunks, seqs=seqs)
        call = pl.pallas_call(
            functools.partial(step_kernel, cfg),
            out_shape=(jax.ShapeDtypeStruct((tp, rows, model), BF16),
                       jax.ShapeDtypeStruct((layers, tp, rows, latent), BF16),
                       jax.ShapeDtypeStruct((layers, tp, rows, 2 * rope), BF16)),
            in_specs=[hb] * 17,
            out_specs=(hb, hb, hb),
            scratch_shapes=scratch,
            compiler_params=pltpu.CompilerParams(collective_id=0, has_side_effects=True, vmem_limit_bytes=67043328),
            name='decode_step',
        )
        x_o, c_o, k_o = call(
            x_in.reshape(tp, rows, model), pos_ids.reshape(1, batch), attn_gain, mlp_gain, q_gain, kv_gain,
            w_dq, w_dkv.transpose(0, 2, 1), w_uq.transpose(0, 2, 3, 1).reshape(layers, heads * per, lora),
            w_uk.reshape(layers, latent * heads, nope), w_uv.reshape(layers, latent * heads, nope),
            w_o.reshape(layers, heads * nope, model),
            w_gate.transpose(0, 2, 1), w_up.transpose(0, 2, 1), w_down,
            ckv_cache, kpe_cache.transpose(0, 1, 3, 2))
        return (x_o.reshape(batch, model), c_o.reshape(layers, batch, latent),
                k_o.reshape(layers, batch, 2 * rope)[..., :rope])

    return jax.shard_map(device_body, mesh=mesh, in_specs=in_specs, out_specs=out_specs, check_vma=False)
```

```python
import math
import functools
import jax
import jax.numpy as jnp
from jax import lax
from jax.experimental import pallas as pl
from jax.experimental.pallas import tpu as pltpu
from jax.sharding import PartitionSpec as P

NORM_EPS = 1e-6
ROPE_BASE = 10000.0
F32 = jnp.float32
BF16 = jnp.bfloat16
MESH = pl.DeviceIdType.MESH
NEG_INF = float('-inf')


def rms(values, gain):
    inv = lax.rsqrt(jnp.mean(values * values, axis=-1, keepdims=True) + NORM_EPS)
    return values * inv * gain


def dot_nt(lhs, rhs):
    return lax.dot_general(lhs, rhs, (((1,), (1,)), ((), ())), preferred_element_type=F32)


def dot_nn(lhs, rhs):
    return jnp.dot(lhs, rhs, preferred_element_type=F32)


def swap_halves(values, half):
    width = values.shape[-1]
    lane = lax.broadcasted_iota(jnp.int32, values.shape, 1)
    up = pltpu.roll(values, half, 1)
    down = pltpu.roll(values, width - half, 1)
    return jnp.where(lane % (2 * half) < half, down, up)


def tile_rows(values, count):
    return jnp.concatenate([values] * count, axis=0)


def step_kernel(cfg, x_hbm, pos_hbm, ag_hbm, mg_hbm, qg_hbm, kg_hbm,
                wdq, wkv, wuq, wuk, wuv, wo, wg, wu, wd, ckv_hbm, kpe_hbm,
                x_out, ckv_out, kpe_out,
                pos_row, ag_ref, mg_ref, qg_ref, kg_ref, cos_ref, sin_ref, pos_ref,
                xb, a_buf, a_pair, acc_in, b_all, q_all, acc_q, u_buf, r_buf, ctx_buf, o_buf, wf,
                gu_acc, act_buf,
                part, d2d, psum, rel, cmb, fin,
                dq_buf, kv_buf, uq_buf, uk_buf, uv_buf, wo_buf, wgu_buf, wd_buf, ckv_buf, kpe_buf, s_buf,
                x_sem, s_sem, px_sem, dq_sem, kv_sem, w_sem, c_sem, out_sem,
                ag_send, ag_recv, rs_send, rs_recv):
    tp_size, layers, heads, kc, slots, chunks, seqs = (
        cfg['tp'], cfg['layers'], cfg['heads'], cfg['kc'], cfg['slots'], cfg['chunks'], cfg['seqs'])
    nchip = tp_size // 2
    model = xb.shape[1]
    rows = xb.shape[0]
    lora = uq_buf.shape[1]
    latent = ckv_buf.shape[-1]
    rope = kpe_buf.shape[2]
    nope = uk_buf.shape[1]
    keys = ckv_buf.shape[2]
    batch = rows * tp_size
    ffn = wd_buf.shape[0]
    cslots = cfg['cslots']
    half_k = model // 2
    n_dq = half_k // kc
    cw = model // chunks
    ch = cw // 2
    scale = float((nope + rope) ** -0.5)

    me = lax.axis_index('tp')
    core = lax.rem(me, 2)
    chip = me // 2
    other = 1 - core
    rchip = lax.rem(chip + 1, nchip)
    lchip = lax.rem(chip + nchip - 1, nchip)
    ochip = lax.rem(chip + 2, nchip)
    mate = 2 * chip + other
    right = 2 * rchip + core
    left = 2 * lchip + core
    opp = 2 * ochip + core

    barrier = pltpu.get_barrier_semaphore()
    for peer in (mate, right, left, opp):
        pl.semaphore_signal(barrier, inc=1, device_id={'tp': peer}, device_id_type=MESH)

    def x_copy():
        return pltpu.make_async_copy(x_hbm.at[me], xb, x_sem)

    def dq_copy(layer, i, slot):
        off = pl.multiple_of(core * half_k + i * kc, 128)
        return pltpu.make_async_copy(wdq.at[layer, pl.ds(off, kc), :], dq_buf.at[slot], dq_sem.at[slot])

    def kv_copy(layer, i, slot):
        off = pl.multiple_of(core * half_k + i * kc, 128)
        return pltpu.make_async_copy(wkv.at[layer, :, pl.ds(off, kc)], kv_buf.at[slot], kv_sem.at[slot])

    weights = [(wuq, uq_buf), (wuk, uk_buf), (wuv, uv_buf), (wo, wo_buf), (wg, wgu_buf.at[0:ffn]), (wu, wgu_buf.at[ffn:2 * ffn]), (wd, wd_buf)]

    def w_copy(layer, idx):
        src, dst = weights[idx]
        return pltpu.make_async_copy(src.at[layer], dst, w_sem.at[idx])

    def ckv_copy(layer, g, slot):
        return pltpu.make_async_copy(ckv_hbm.at[layer, pl.ds(g * seqs, seqs)], ckv_buf.at[slot], c_sem.at[0, slot])

    def kpe_copy(layer, g, slot):
        return pltpu.make_async_copy(kpe_hbm.at[layer, pl.ds(g * seqs, seqs)], kpe_buf.at[slot], c_sem.at[1, slot])

    def start_dq(layer):
        for s in range(slots):
            dq_copy(layer, s, s).start()
            kv_copy(layer, s, s).start()

    def start_cache(layer):
        for s in range(cslots):
            ckv_copy(layer, s, s).start()
            kpe_copy(layer, s, s).start()

    def remote(src, dst, sems, recvs, j, kind, dev):
        return pltpu.make_async_remote_copy(src_ref=src, dst_ref=dst, send_sem=sems.at[j, kind],
                                            recv_sem=recvs.at[j, kind], device_id={'tp': dev}, device_id_type=MESH)

    def ag_desc(buf, j, spec, kind, blk, dev):
        off, half_a, width, direct = spec
        lo, size = off, width
        if not direct and kind in (3, 7):
            size = half_a
        elif not direct and kind in (4, 8):
            lo, size = off + half_a, width - half_a
        ref = buf.at[blk, :, pl.ds(lo, size)]
        return remote(ref, ref, ag_send, ag_recv, j, kind, dev)

    mleft = 2 * lchip + other
    mright = 2 * rchip + other
    mopp = 2 * ochip + other
    ag_out = [(me, mate), (me, right), (me, left), (left, right), (right, left), (left, mate), (right, mate), (opp, mate), (opp, mate)]
    ag_in = [mate, left, right, opp, opp, mleft, mright, mopp, mopp]

    def ag_route(spec, kind):
        if kind == 3 and spec[3]:
            return me, opp
        return ag_out[kind]

    def ag_start(buf, j, spec, kind):
        ag_desc(buf, j, spec, kind, *ag_route(spec, kind)).start()

    def ag_wait(buf, j, spec, kind):
        ag_desc(buf, j, spec, kind, ag_in[kind], mate).wait_recv()

    def all_gather(buf, specs, consume):
        n = len(specs)
        for j in range(n):
            for kind in ((1, 2, 3, 0) if specs[j][3] else (1, 2, 0)):
                ag_start(buf, j, specs[j], kind)

        def forward(j):
            direct = specs[j][3]
            for kind in (1, 2):
                ag_wait(buf, j, specs[j], kind)
                if not direct:
                    ag_start(buf, j, specs[j], kind + 2)
                ag_start(buf, j, specs[j], kind + 4)

        def pass_far(j):
            for kind in ((3,) if specs[j][3] else (3, 4)):
                ag_wait(buf, j, specs[j], kind)
                ag_start(buf, j, specs[j], kind + 4)

        def finish(j):
            for kind in ((0, 5, 6, 7) if specs[j][3] else (0, 5, 6, 7, 8)):
                ag_wait(buf, j, specs[j], kind)
            with jax.named_scope('consume'):
                consume(j)

        lead = sum(spec[3] for spec in specs)
        if n == 1:
            lead = 0
        for j in range(n):
            forward(j)
            if 1 <= j <= lead:
                pass_far(j - 1)
            if 2 <= j <= lead + 1:
                finish(j - 2)
        if lead:
            for j in range(max(n - 2, 0), lead):
                finish(j)
        pass_far(lead)
        for j in range(lead, n):
            if j + 1 < n:
                pass_far(j + 1)
            finish(j)
        for j in range(n):
            for kind in range(9):
                if not (specs[j][3] and kind in (4, 8)):
                    ag_desc(buf, j, specs[j], kind, *ag_route(specs[j], kind)).wait_send()

    def rs_desc(j, kind):
        o = j * cw
        ca, cb = pl.ds(o, ch), pl.ds(o + ch, ch)
        hj = pl.ds(j * ch, ch)
        full = pl.ds(o, cw)
        src, dst, dev = [
            lambda: (part.at[:, other, :, full], d2d.at[:, :, full], mate),
            lambda: (psum.at[ochip, :, ca], rel.at[0, :, hj], right),
            lambda: (psum.at[ochip, :, cb], rel.at[1, :, hj], left),
            lambda: (psum.at[rchip, :, cb], fin.at[0, :, cb], right),
            lambda: (psum.at[lchip, :, ca], fin.at[1, :, ca], left),
            lambda: (cmb.at[0, :, hj], fin.at[0, :, ca], right),
            lambda: (cmb.at[1, :, hj], fin.at[1, :, cb], left),
        ][kind]()
        return remote(src, dst, rs_send, rs_recv, j, kind, dev)

    def reduce_scatter(product):
        def mm(j):
            val = product(j)
            part[:, :, :, pl.ds(j * cw, cw)] = val.reshape(nchip, 2, rows, cw).astype(BF16)
            rs_desc(j, 0).start()

        def pair(j):
            rs_desc(j, 0).wait_recv()
            cols = pl.ds(j * cw, cw)
            psum[ochip, :, cols] = (part[ochip, core, :, cols].astype(F32) + d2d[ochip, :, cols].astype(F32)).astype(BF16)
            rs_desc(j, 1).start()
            rs_desc(j, 2).start()
            for cc in (rchip, lchip, chip):
                psum[cc, :, cols] = (part[cc, core, :, cols].astype(F32) + d2d[cc, :, cols].astype(F32)).astype(BF16)

        def combine(j):
            o = j * cw
            hj = pl.ds(j * ch, ch)
            rs_desc(j, 1).wait_recv()
            cmb[0, :, hj] = (psum[rchip, :, pl.ds(o, ch)].astype(F32) + rel[0, :, hj].astype(F32)).astype(BF16)
            rs_desc(j, 5).start()
            rs_desc(j, 2).wait_recv()
            cmb[1, :, hj] = (psum[lchip, :, pl.ds(o + ch, ch)].astype(F32) + rel[1, :, hj].astype(F32)).astype(BF16)
            rs_desc(j, 6).start()

        def final(j):
            for kind in (3, 4, 5, 6):
                rs_desc(j, kind).wait_recv()
            cols = pl.ds(j * cw, cw)
            total = psum[chip, :, cols].astype(F32) + fin[0, :, cols].astype(F32) + fin[1, :, cols].astype(F32)
            xb[:, cols] = (xb[:, cols].astype(F32) + total).astype(BF16)

        for j in range(chunks + 1):
            if j < chunks:
                mm(j)
            if j > 0:
                pair(j - 1)
        for j in range(chunks):
            rs_desc(j, 3).start()
            rs_desc(j, 4).start()
        for j in range(chunks):
            combine(j)
        return final

    def rs_drain(final):
        for j in range(chunks):
            final(j)
        for j in range(chunks):
            for kind in range(7):
                rs_desc(j, kind).wait_send()

    gchunks = cfg['gchunks']
    gw = model // gchunks
    gh = (gw // 128 + 1) // 2 * 128
    b_specs = [(j * gw, gh, gw, j < cfg['direct']) for j in range(gchunks)]
    x_specs = [(j * gw, gh, gw, False) for j in range(gchunks)]
    qw = q_all.shape[2]
    q_specs = [(0, 0, qw, True)]

    def gain_row(ref, layer):
        vals = ref[...].astype(F32)
        row = vals[0:1]
        for i in range(1, layers):
            row = jnp.where(layer == i, vals[i:i + 1], row)
        return row

    small = [(pos_hbm, pos_row), (ag_hbm, ag_ref), (mg_hbm, mg_ref), (qg_hbm, qg_ref), (kg_hbm, kg_ref)]
    x_copy().start()
    for i, (src, dst) in enumerate(small):
        pltpu.make_async_copy(src, dst, s_sem.at[i]).start()
    start_dq(0)
    for i, (src, dst) in enumerate(small):
        pltpu.make_async_copy(src, dst, s_sem.at[i]).wait()
    pos_f = jnp.transpose(jnp.broadcast_to(pos_row[...].astype(F32), (batch, batch)))
    pos_ref[...] = pos_f.astype(jnp.int32)
    lane_f = lax.broadcasted_iota(jnp.int32, (batch, batch), 1) % (rope // 2)
    angles = pos_f * jnp.exp(lane_f.astype(F32) * (-2.0 * math.log(ROPE_BASE) / rope))
    cos_v, sin_v = jnp.cos(angles), jnp.sin(angles)
    lane_s = lax.broadcasted_iota(jnp.int32, (batch, batch), 1) % rope
    sin_v = jnp.where(lane_s < rope // 2, -sin_v, sin_v)
    for i in range(heads * rope // batch):
        cos_ref[:, i * batch:(i + 1) * batch] = cos_v
        sin_ref[:, i * batch:(i + 1) * batch] = sin_v
    x_copy().wait()

    def pair_copy(src, dst, i):
        return pltpu.make_async_remote_copy(src_ref=src, dst_ref=dst, send_sem=px_sem.at[0, i], recv_sem=px_sem.at[1, i],
                                            device_id={'tp': mate}, device_id_type=MESH)

    def layer_body(layer, carry):
        more = layer + 1 < layers
        a_buf[...] = rms(xb[...].astype(F32), gain_row(ag_ref, layer)).astype(BF16)

        @pl.when(layer == 0)
        def _():
            pl.semaphore_wait(barrier, 4)

        swap = pair_copy(a_buf.at[:, pl.ds(pl.multiple_of(other * half_k, 128), half_k)], a_pair.at[1], 0)
        swap.start()
        a_pair[0] = a_buf[:, pl.ds(pl.multiple_of(core * half_k, 128), half_k)]
        acc_q[...] = jnp.zeros_like(acc_q)
        swap.wait_recv()

        def dq_step(i, c):
            slot = lax.rem(i, slots)
            dq_copy(layer, i, slot).wait()
            kv_copy(layer, i, slot).wait()
            a_c = a_pair[:, :, pl.ds(pl.multiple_of(i * kc, 128), kc)].reshape(2 * rows, kc)
            acc_q[:, :, 0:lora] += dot_nn(a_c, dq_buf[slot]).reshape(2, rows, lora)
            acc_q[:, :, lora:lora + latent + rope] += dot_nt(a_c, kv_buf[slot]).reshape(2, rows, latent + rope)

            @pl.when(i + slots < n_dq)
            def _():
                dq_copy(layer, i + slots, slot).start()
                kv_copy(layer, i + slots, slot).start()
            return c

        lax.fori_loop(0, n_dq, dq_step, 0)

        @pl.when(layer == 0)
        def _():
            for idx in (0, 1, 2):
                w_copy(layer, idx).start()
            start_cache(layer)
            w_copy(layer, 3).start()

        back = pair_copy(acc_q.at[1], acc_in, 1)
        back.start()
        back.wait_recv()
        lat = acc_q[0] + acc_in[...]
        q_all[me, :, pl.ds(0, lora)] = rms(lat[:, :lora], gain_row(qg_ref, layer)).astype(BF16)
        kv = lat[:, lora:]
        q_all[me, :, pl.ds(lora, latent)] = rms(kv[:, :latent], gain_row(kg_ref, layer)).astype(BF16)
        row0 = pl.multiple_of(me * rows, rows)
        kr = kv[:, latent:latent + rope]
        kr = jnp.concatenate([kr, kr], axis=1)
        kr = kr * cos_ref[pl.ds(row0, rows), 0:2 * rope] + swap_halves(kr, rope // 2) * sin_ref[pl.ds(row0, rows), 0:2 * rope]
        lane = lax.broadcasted_iota(jnp.int32, kr.shape, 1)
        q_all[me, :, pl.ds(lora + latent, 2 * rope)] = jnp.where(lane < rope, kr, 0.0).astype(BF16)

        def nothing(j):
            return None

        swap.wait_send()
        back.wait_send()
        all_gather(q_all, q_specs, nothing)

        out_c = pltpu.make_async_copy(q_all.at[:, :, pl.ds(lora, latent)], ckv_out.at[layer], out_sem.at[0])
        out_k = pltpu.make_async_copy(q_all.at[:, :, pl.ds(lora + latent, 2 * rope)], kpe_out.at[layer], out_sem.at[1])
        out_c.start()
        out_k.start()

        w_copy(layer, 0).wait()
        c_q = q_all[:, :, pl.ds(0, lora)].reshape(batch, lora)
        per = nope + rope
        w_n = jnp.concatenate([uq_buf[pl.ds(h * per, nope), :] for h in range(heads)], axis=0)
        w_r = jnp.concatenate([uq_buf[pl.ds(h * per + nope, rope), :] for h in range(heads)], axis=0)
        q_n = dot_nt(c_q, w_n).astype(BF16)
        q_r = dot_nt(c_q, w_r)
        q_r = q_r * cos_ref[...] + swap_halves(q_r, rope // 2) * sin_ref[...]
        lane2 = lax.broadcasted_iota(jnp.int32, (batch, 2 * rope), 1)
        for pair_i in range(heads // 2):
            duo = q_r[:, pair_i * 2 * rope:(pair_i + 1) * 2 * rope]
            swp = pltpu.roll(duo, rope, 1)
            r_buf[2 * pair_i] = jnp.where(lane2 < rope, duo, swp).astype(BF16)
            r_buf[2 * pair_i + 1] = jnp.where(lane2 < rope, swp, duo).astype(BF16)
        w_copy(layer, 1).wait()
        wf[...] = uk_buf[...].astype(F32)
        for h in range(heads):
            wk_h = wf[pl.ds(h, latent, stride=heads), :].astype(BF16)
            u_buf[h] = dot_nt(q_n[:, h * nope:(h + 1) * nope], wk_h).astype(BF16)

        @pl.when(more)
        def _():
            w_copy(layer + 1, 0).start()
            w_copy(layer + 1, 1).start()

        m_rows = heads * seqs

        groups = batch // seqs
        row_b = lax.broadcasted_iota(jnp.int32, (m_rows, keys), 0) % seqs
        lane_k = lax.broadcasted_iota(jnp.int32, (m_rows, keys), 1)
        lane_r = lax.broadcasted_iota(jnp.int32, (m_rows, 2 * rope), 1) // rope

        def att_wait(g):
            slot = lax.rem(g, cslots)
            ckv_copy(layer, g, slot).wait()
            kpe_copy(layer, g, slot).wait()

        def scores(g):
            slot = lax.rem(g, cslots)
            r0 = pl.multiple_of(g * seqs, seqs)
            u_g = u_buf[:, pl.ds(r0, seqs), :].reshape(m_rows, latent)
            r_g = r_buf[:, pl.ds(r0, seqs), :].reshape(m_rows, 2 * rope).astype(F32)
            s_t = dot_nt(u_g, ckv_buf[slot].reshape(seqs * keys, latent))
            s_n = s_t[:, 0:keys]
            for b in range(1, seqs):
                s_n = jnp.where(row_b == b, s_t[:, b * keys:(b + 1) * keys], s_n)
            q_blk = jnp.concatenate(
                [jnp.where(row_b == 2 * b + lane_r, r_g, 0.0).astype(BF16) for b in range(seqs // 2)], axis=1)
            s_r = dot_nn(q_blk, kpe_buf[slot].reshape(seqs * rope, keys))
            cn = tile_rows(q_all[g, :, pl.ds(lora, latent)].astype(F32), heads)
            kn = tile_rows(q_all[g, :, pl.ds(lora + latent, 2 * rope)].astype(F32), heads)
            fresh = jnp.sum(u_g.astype(F32) * cn, axis=-1, keepdims=True) + jnp.sum(r_g * kn, axis=-1, keepdims=True)
            pos = tile_rows(pos_ref[pl.ds(r0, seqs), :], heads)
            s = jnp.where(lane_k == pos, fresh, s_n + s_r) * scale
            return jnp.where(lane_k <= pos, s, NEG_INF)

        def context(g, s):
            slot = lax.rem(g, cslots)
            r0 = pl.multiple_of(g * seqs, seqs)
            e = jnp.exp(s - jnp.max(s, axis=-1, keepdims=True))
            prob = (e / jnp.sum(e, axis=-1, keepdims=True)).astype(BF16).astype(F32)
            at_pos = lane_k == tile_rows(pos_ref[pl.ds(r0, seqs), :], heads)
            p_new = jnp.sum(jnp.where(at_pos, prob, 0.0), axis=-1, keepdims=True)
            p_old = jnp.where(at_pos, 0.0, prob)
            p_blk = jnp.concatenate([jnp.where(row_b == b, p_old, 0.0).astype(BF16) for b in range(seqs)], axis=1)
            cn = tile_rows(q_all[g, :, pl.ds(lora, latent)].astype(F32), heads)
            ctx = dot_nn(p_blk, ckv_buf[slot].reshape(seqs * keys, latent)) + p_new * cn
            ctx_buf[:, pl.ds(r0, seqs), :] = ctx.astype(BF16).reshape(heads, seqs, latent)

        att_wait(0)
        s_buf[...] = scores(0)

        def att_step(g, c):
            att_wait(g + 1)
            s_now = s_buf[...]
            s_next = scores(g + 1)
            context(g, s_now)
            s_buf[...] = s_next

            @pl.when(g + cslots < groups)
            def _():
                slot = lax.rem(g, cslots)
                ckv_copy(layer, g + cslots, slot).start()
                kpe_copy(layer, g + cslots, slot).start()
            return c

        lax.fori_loop(0, groups - 1, att_step, 0)

        @pl.when(layer == 0)
        def _():
            for idx in (4, 5, 6):
                w_copy(layer, idx).start()

        context(groups - 1, s_buf[...])

        w_copy(layer, 2).wait()
        wf[...] = uv_buf[...].astype(F32)
        for h in range(heads):
            wv_h = wf[pl.ds(h, latent, stride=heads), :].astype(BF16)
            o_buf[:, h * nope:(h + 1) * nope] = dot_nn(ctx_buf[h], wv_h).astype(BF16)

        @pl.when(more)
        def _():
            w_copy(layer + 1, 2).start()

        w_copy(layer, 3).wait()
        out_c.wait()
        out_k.wait()

        final = reduce_scatter(lambda j: dot_nn(o_buf[...], wo_buf[:, pl.ds(j * cw, cw)]))

        @pl.when(more)
        def _():
            start_dq(layer + 1)
            start_cache(layer + 1)
            w_copy(layer + 1, 3).start()

        rs_drain(final)

        b_all[me] = rms(xb[...].astype(F32), gain_row(mg_ref, layer)).astype(BF16)
        w_copy(layer, 4).wait()
        w_copy(layer, 5).wait()

        def gate_up(j):
            cols = pl.ds(j * gw, gw)
            b_c = b_all[:, :, cols].reshape(batch, gw)
            val = dot_nt(b_c, wgu_buf[:, cols])
            if j == 0:
                gu_acc[...] = val
            else:
                gu_acc[...] += val

        all_gather(b_all, b_specs, gate_up)
        gate = gu_acc[:, 0:ffn]
        act_buf[...] = (gate * lax.logistic(gate) * gu_acc[:, ffn:2 * ffn]).astype(BF16)
        w_copy(layer, 6).wait()

        @pl.when(more)
        def _():
            w_copy(layer + 1, 4).start()
            w_copy(layer + 1, 5).start()

        final2 = reduce_scatter(lambda j: dot_nn(act_buf[...], wd_buf[:, pl.ds(j * cw, cw)]))

        @pl.when(more)
        def _():
            w_copy(layer + 1, 6).start()

        rs_drain(final2)
        return carry

    lax.fori_loop(0, layers, layer_body, 0)

    b_all[me] = xb[...]

    def put(j):
        cols = pl.ds(j * gw, gw)
        pltpu.make_async_copy(b_all.at[:, :, cols], x_out.at[:, :, cols], out_sem.at[j]).start()

    all_gather(b_all, x_specs, put)
    for j in range(gchunks):
        cols = pl.ds(j * gw, gw)
        pltpu.make_async_copy(b_all.at[:, :, cols], x_out.at[:, :, cols], out_sem.at[j]).wait()


def solution(mesh):
    tp = mesh.shape['tp']
    cache_spec = P(None, 'dp', None, None)
    head_spec = P(None, None, 'tp', None)
    weight_specs = (P(), P(), P(), P(), P(), head_spec, head_spec, head_spec, P(None, 'tp', None, None), P(), P(None, None, 'tp'), P(None, None, 'tp'), P(None, 'tp', None))
    in_specs = (P('dp', None), P('dp'), cache_spec, cache_spec) + weight_specs
    out_specs = (P('dp', None), P(None, 'dp', None), P(None, 'dp', None))

    def device_body(x_in, pos_ids, ckv_cache, kpe_cache, attn_gain, w_dq, q_gain, w_dkv, kv_gain, w_uq, w_uk, w_uv, w_o,
                    mlp_gain, w_gate, w_up, w_down):
        batch, model = x_in.shape
        layers, _, keys, latent = ckv_cache.shape
        rope = kpe_cache.shape[-1]
        lora = w_dq.shape[-1]
        heads, per = w_uq.shape[2:]
        nope = w_uk.shape[-1]
        ffn = w_gate.shape[-1]
        rows = batch // tp
        kc, slots, chunks, gchunks, direct, seqs, cslots = 512, 3, 4, 4, 1, rows, 3
        hb = pl.BlockSpec(memory_space=pl.ANY)
        dma = pltpu.SemaphoreType.DMA
        qw = lora + latent + 2 * rope
        ch = model // chunks // 2
        scratch = [
            pltpu.VMEM((1, batch), jnp.int32),
            pltpu.VMEM((layers, model), BF16),
            pltpu.VMEM((layers, model), BF16),
            pltpu.VMEM((layers, lora), BF16),
            pltpu.VMEM((layers, latent), BF16),
            pltpu.VMEM((batch, heads * rope), F32),
            pltpu.VMEM((batch, heads * rope), F32),
            pltpu.VMEM((batch, keys), jnp.int32),
            pltpu.VMEM((rows, model), BF16),
            pltpu.VMEM((rows, model), BF16),
            pltpu.VMEM((2, rows, model // 2), BF16),
            pltpu.VMEM((rows, lora + latent + 2 * rope), F32),
            pltpu.VMEM((tp, rows, model), BF16),
            pltpu.VMEM((tp, rows, qw), BF16),
            pltpu.VMEM((2, rows, lora + latent + 2 * rope), F32),
            pltpu.VMEM((heads, batch, latent), BF16),
            pltpu.VMEM((heads, batch, 2 * rope), BF16),
            pltpu.VMEM((heads, batch, latent), BF16),
            pltpu.VMEM((batch, heads * nope), BF16),
            pltpu.VMEM((latent * heads, nope), F32),
            pltpu.VMEM((batch, 2 * ffn), F32),
            pltpu.VMEM((batch, ffn), BF16),
            pltpu.VMEM((tp // 2, 2, rows, model), BF16),
            pltpu.VMEM((tp // 2, rows, model), BF16),
            pltpu.VMEM((tp // 2, rows, model), BF16),
            pltpu.VMEM((2, rows, model // 2), BF16),
            pltpu.VMEM((2, rows, model // 2), BF16),
            pltpu.VMEM((2, rows, model), BF16),
            pltpu.VMEM((slots, kc, lora), BF16),
            pltpu.VMEM((slots, latent + rope, kc), BF16),
            pltpu.VMEM((heads * per, lora), BF16),
            pltpu.VMEM((latent * heads, nope), BF16),
            pltpu.VMEM((latent * heads, nope), BF16),
            pltpu.VMEM((heads * nope, model), BF16),
            pltpu.VMEM((2 * ffn, model), BF16),
            pltpu.VMEM((ffn, model), BF16),
            pltpu.VMEM((cslots, seqs, keys, latent), BF16),
            pltpu.VMEM((cslots, seqs, rope, keys), BF16),
            pltpu.VMEM((heads * seqs, keys), F32),
            dma(()), dma((5,)), dma((2, 2)), dma((slots,)), dma((slots,)), dma((7,)), dma((2, cslots)), dma((gchunks,)),
            dma((gchunks, 9)), dma((gchunks, 9)), dma((chunks, 7)), dma((chunks, 7)),
        ]
        cfg = dict(tp=tp, layers=layers, heads=heads, kc=kc, slots=slots, chunks=chunks, seqs=seqs, cslots=cslots, gchunks=gchunks, direct=direct)
        call = pl.pallas_call(
            functools.partial(step_kernel, cfg),
            out_shape=(jax.ShapeDtypeStruct((tp, rows, model), BF16),
                       jax.ShapeDtypeStruct((layers, tp, rows, latent), BF16),
                       jax.ShapeDtypeStruct((layers, tp, rows, 2 * rope), BF16)),
            in_specs=[hb] * 17,
            out_specs=(hb, hb, hb),
            scratch_shapes=scratch,
            compiler_params=pltpu.CompilerParams(collective_id=0, has_side_effects=True, vmem_limit_bytes=67043328),
            name='decode_step',
        )
        x_o, c_o, k_o = call(
            x_in.reshape(tp, rows, model), pos_ids.reshape(1, batch), attn_gain, mlp_gain, q_gain, kv_gain,
            w_dq, w_dkv.transpose(0, 2, 1), w_uq.transpose(0, 2, 3, 1).reshape(layers, heads * per, lora),
            w_uk.reshape(layers, latent * heads, nope), w_uv.reshape(layers, latent * heads, nope),
            w_o.reshape(layers, heads * nope, model),
            w_gate.transpose(0, 2, 1), w_up.transpose(0, 2, 1), w_down,
            ckv_cache, kpe_cache.transpose(0, 1, 3, 2))
        return (x_o.reshape(batch, model), c_o.reshape(layers, batch, latent),
                k_o.reshape(layers, batch, 2 * rope)[..., :rope])

    return jax.shard_map(device_body, mesh=mesh, in_specs=in_specs, out_specs=out_specs, check_vma=False)
```

```python
import math
import functools
import jax
import jax.numpy as jnp
from jax import lax
from jax.experimental import pallas as pl
from jax.experimental.pallas import tpu as pltpu
from jax.sharding import PartitionSpec as P

NORM_EPS = 1e-6
ROPE_BASE = 10000.0
F32 = jnp.float32
BF16 = jnp.bfloat16
MESH = pl.DeviceIdType.MESH
NEG_INF = float('-inf')


def rms(values, gain):
    inv = lax.rsqrt(jnp.mean(values * values, axis=-1, keepdims=True) + NORM_EPS)
    return values * inv * gain


def dot_nt(lhs, rhs):
    return lax.dot_general(lhs, rhs, (((1,), (1,)), ((), ())), preferred_element_type=F32)


def dot_nn(lhs, rhs):
    return jnp.dot(lhs, rhs, preferred_element_type=F32)


def swap_halves(values, half):
    width = values.shape[-1]
    lane = lax.broadcasted_iota(jnp.int32, values.shape, 1)
    up = pltpu.roll(values, half, 1)
    down = pltpu.roll(values, width - half, 1)
    return jnp.where(lane % (2 * half) < half, down, up)


def tile_rows(values, count):
    return jnp.concatenate([values] * count, axis=0)


def step_kernel(cfg, x_hbm, pos_hbm, ag_hbm, mg_hbm, qg_hbm, kg_hbm,
                wdq, wkv, wuq, wuk, wuv, wo, wg, wu, wd, ckv_hbm, kpe_hbm,
                x_out, ckv_out, kpe_out,
                pos_row, ag_ref, mg_ref, qg_ref, kg_ref, cos_ref, sin_ref, pos_ref,
                xb, a_buf, a_pair, acc_in, b_all, q_all, acc_q, acc_all, acc_rcv, u_buf, r_buf, u_in, r_in, ctx_buf, ctx_out, o_buf, wf,
                gu_acc, act_buf,
                part, d2d, psum, rel, cmb, fin,
                dq_buf, kv_buf, uq_buf, uk_buf, uv_buf, wo_buf, wgu_buf, wd_buf, ckv_buf, kpe_buf, s_buf,
                x_sem, s_sem, px_sem, hx_sem, cx_sem, dq_sem, kv_sem, w_sem, c_sem, out_sem,
                ag_send, ag_recv, rs_send, rs_recv):
    tp_size, layers, heads, kc, slots, chunks, seqs = (
        cfg['tp'], cfg['layers'], cfg['heads'], cfg['kc'], cfg['slots'], cfg['chunks'], cfg['seqs'])
    nchip = tp_size // 2
    model = xb.shape[1]
    rows = xb.shape[0]
    lora = uq_buf.shape[1]
    latent = ckv_buf.shape[-1]
    rope = kpe_buf.shape[2]
    nope = uk_buf.shape[1]
    keys = ckv_buf.shape[2]
    batch = rows * tp_size
    ffn = wd_buf.shape[0]
    cslots = cfg['cslots']
    half_k = model // 2
    n_dq = half_k // kc
    cw = model // chunks
    ch = cw // 2
    scale = float((nope + rope) ** -0.5)

    me = lax.axis_index('tp')
    core = lax.rem(me, 2)
    chip = me // 2
    other = 1 - core
    rchip = lax.rem(chip + 1, nchip)
    lchip = lax.rem(chip + nchip - 1, nchip)
    ochip = lax.rem(chip + 2, nchip)
    mate = 2 * chip + other
    right = 2 * rchip + core
    left = 2 * lchip + core
    opp = 2 * ochip + core

    barrier = pltpu.get_barrier_semaphore()
    for peer in (mate, right, left, opp):
        pl.semaphore_signal(barrier, inc=1, device_id={'tp': peer}, device_id_type=MESH)

    def x_copy():
        return pltpu.make_async_copy(x_hbm.at[me], xb, x_sem.at[0])

    def dq_copy(layer, i, slot):
        off = pl.multiple_of(core * half_k + i * kc, 128)
        return pltpu.make_async_copy(wdq.at[layer, pl.ds(off, kc), :], dq_buf.at[slot], dq_sem.at[slot])

    def kv_copy(layer, i, slot):
        off = pl.multiple_of(core * half_k + i * kc, 128)
        return pltpu.make_async_copy(wkv.at[layer, :, pl.ds(off, kc)], kv_buf.at[slot], kv_sem.at[slot])

    weights = [(wuq, uq_buf), (wuk, uk_buf), (wuv, uv_buf), (wo, wo_buf), (wg, wgu_buf.at[0:ffn]), (wu, wgu_buf.at[ffn:2 * ffn]), (wd, wd_buf)]

    def w_copy(layer, idx):
        src, dst = weights[idx]
        return pltpu.make_async_copy(src.at[layer], dst, w_sem.at[idx])

    def ckv_copy(layer, g, slot):
        return pltpu.make_async_copy(ckv_hbm.at[layer, pl.ds(core * (batch // 2) + g * seqs, seqs)], ckv_buf.at[slot], c_sem.at[0, slot])

    def kpe_copy(layer, g, slot):
        return pltpu.make_async_copy(kpe_hbm.at[layer, pl.ds(core * (batch // 2) + g * seqs, seqs)], kpe_buf.at[slot], c_sem.at[1, slot])

    def start_dq(layer):
        for s in range(slots):
            dq_copy(layer, s, s).start()
            kv_copy(layer, s, s).start()

    def start_cache(layer):
        for s in range(cslots):
            ckv_copy(layer, s, s).start()
            kpe_copy(layer, s, s).start()

    def remote(src, dst, sems, recvs, j, kind, dev):
        return pltpu.make_async_remote_copy(src_ref=src, dst_ref=dst, send_sem=sems.at[j, kind],
                                            recv_sem=recvs.at[j, kind], device_id={'tp': dev}, device_id_type=MESH)

    def ag_desc(buf, j, spec, kind, blk, dev):
        off, half_a, width, direct = spec
        lo, size = off, width
        if not direct and kind in (3, 7):
            size = half_a
        elif not direct and kind in (4, 8):
            lo, size = off + half_a, width - half_a
        ref = buf.at[blk, :, pl.ds(lo, size)]
        return remote(ref, ref, ag_send, ag_recv, j, kind, dev)

    mleft = 2 * lchip + other
    mright = 2 * rchip + other
    mopp = 2 * ochip + other
    ag_out = [(me, mate), (me, right), (me, left), (left, right), (right, left), (left, mate), (right, mate), (opp, mate), (opp, mate)]
    ag_in = [mate, left, right, opp, opp, mleft, mright, mopp, mopp]

    def ag_route(spec, kind):
        if kind == 3 and spec[3]:
            return me, opp
        return ag_out[kind]

    def ag_start(buf, j, spec, kind):
        ag_desc(buf, j, spec, kind, *ag_route(spec, kind)).start()

    def ag_wait(buf, j, spec, kind):
        ag_desc(buf, j, spec, kind, ag_in[kind], mate).wait_recv()

    def ag_first(buf, j, spec):
        for kind in ((1, 2, 3, 0) if spec[3] else (1, 2, 0)):
            ag_start(buf, j, spec, kind)

    def all_gather(buf, specs, consume, started=False):
        n = len(specs)
        for j in range(n):
            if not started:
                ag_first(buf, j, specs[j])

        def forward(j):
            direct = specs[j][3]
            for kind in (1, 2):
                ag_wait(buf, j, specs[j], kind)
                if not direct:
                    ag_start(buf, j, specs[j], kind + 2)
                ag_start(buf, j, specs[j], kind + 4)

        def pass_far(j):
            for kind in ((3,) if specs[j][3] else (3, 4)):
                ag_wait(buf, j, specs[j], kind)
                ag_start(buf, j, specs[j], kind + 4)

        def finish(j):
            for kind in ((0, 5, 6, 7) if specs[j][3] else (0, 5, 6, 7, 8)):
                ag_wait(buf, j, specs[j], kind)
            with jax.named_scope('consume'):
                consume(j)

        lead = sum(spec[3] for spec in specs)
        if n == 1:
            lead = 0
        for j in range(n):
            forward(j)
            if 1 <= j <= lead:
                pass_far(j - 1)
            if 2 <= j <= lead + 1:
                finish(j - 2)
        if lead:
            for j in range(max(n - 2, 0), lead):
                finish(j)
        pass_far(lead)
        for j in range(lead, n):
            if j + 1 < n:
                pass_far(j + 1)
            finish(j)
        for j in range(n):
            for kind in range(9):
                if not (specs[j][3] and kind in (4, 8)):
                    ag_desc(buf, j, specs[j], kind, *ag_route(specs[j], kind)).wait_send()

    def rs_desc(j, kind):
        o = j * cw
        ca, cb = pl.ds(o, ch), pl.ds(o + ch, ch)
        hj = pl.ds(j * ch, ch)
        full = pl.ds(o, cw)
        src, dst, dev = [
            lambda: (part.at[:, other, :, full], d2d.at[:, :, full], mate),
            lambda: (psum.at[ochip, :, ca], rel.at[0, :, hj], right),
            lambda: (psum.at[ochip, :, cb], rel.at[1, :, hj], left),
            lambda: (psum.at[rchip, :, cb], fin.at[0, :, cb], right),
            lambda: (psum.at[lchip, :, ca], fin.at[1, :, ca], left),
            lambda: (cmb.at[0, :, hj], fin.at[0, :, ca], right),
            lambda: (cmb.at[1, :, hj], fin.at[1, :, cb], left),
        ][kind]()
        return remote(src, dst, rs_send, rs_recv, j, kind, dev)

    def reduce_scatter(product):
        def mm(j):
            val = product(j)
            part[:, :, :, pl.ds(j * cw, cw)] = val.reshape(nchip, 2, rows, cw).astype(BF16)
            rs_desc(j, 0).start()

        def pair(j):
            rs_desc(j, 0).wait_recv()
            cols = pl.ds(j * cw, cw)
            psum[ochip, :, cols] = (part[ochip, core, :, cols].astype(F32) + d2d[ochip, :, cols].astype(F32)).astype(BF16)
            rs_desc(j, 1).start()
            rs_desc(j, 2).start()
            for cc in (rchip, lchip, chip):
                psum[cc, :, cols] = (part[cc, core, :, cols].astype(F32) + d2d[cc, :, cols].astype(F32)).astype(BF16)

        def combine(j):
            o = j * cw
            hj = pl.ds(j * ch, ch)
            rs_desc(j, 1).wait_recv()
            cmb[0, :, hj] = (psum[rchip, :, pl.ds(o, ch)].astype(F32) + rel[0, :, hj].astype(F32)).astype(BF16)
            rs_desc(j, 5).start()
            rs_desc(j, 2).wait_recv()
            cmb[1, :, hj] = (psum[lchip, :, pl.ds(o + ch, ch)].astype(F32) + rel[1, :, hj].astype(F32)).astype(BF16)
            rs_desc(j, 6).start()

        def final(j):
            for kind in (3, 4, 5, 6):
                rs_desc(j, kind).wait_recv()
            cols = pl.ds(j * cw, cw)
            total = psum[chip, :, cols].astype(F32) + fin[0, :, cols].astype(F32) + fin[1, :, cols].astype(F32)
            xb[:, cols] = (xb[:, cols].astype(F32) + total).astype(BF16)

        for j in range(chunks + 1):
            if j < chunks:
                mm(j)
            if j > 0:
                pair(j - 1)
        for j in range(chunks):
            rs_desc(j, 3).start()
            rs_desc(j, 4).start()
        for j in range(chunks):
            combine(j)
        return final

    def rs_drain(final, hook=None):
        for j in range(chunks):
            final(j)
            if hook is not None:
                hook(j)
        for j in range(chunks):
            for kind in range(7):
                rs_desc(j, kind).wait_send()

    gchunks = cfg['gchunks']
    gw = model // gchunks
    gh = (gw // 128 + 1) // 2 * 128
    b_specs = [(j * gw, gh, gw, j < cfg['direct']) for j in range(gchunks)]
    x_specs = [(j * cw, ch, cw, False) for j in range(chunks)]
    qw = q_all.shape[2]
    q_specs = [(0, 0, qw, True)]

    def gain_row(ref, layer):
        vals = ref[...].astype(F32)
        row = vals[0:1]
        for i in range(1, layers):
            row = jnp.where(layer == i, vals[i:i + 1], row)
        return row

    small = [(pos_hbm, pos_row), (ag_hbm, ag_ref), (mg_hbm, mg_ref), (qg_hbm, qg_ref), (kg_hbm, kg_ref)]
    x_all = pltpu.make_async_copy(x_hbm, b_all, x_sem.at[1])
    x_all.start()
    x_copy().start()
    for i, (src, dst) in enumerate(small):
        pltpu.make_async_copy(src, dst, s_sem.at[i]).start()
    start_dq(0)
    for i, (src, dst) in enumerate(small):
        pltpu.make_async_copy(src, dst, s_sem.at[i]).wait()
    pos_f = jnp.transpose(jnp.broadcast_to(pos_row[...].astype(F32), (batch, batch)))
    pos_ref[...] = pos_f.astype(jnp.int32)
    lane_f = lax.broadcasted_iota(jnp.int32, (batch, batch), 1) % (rope // 2)
    angles = pos_f * jnp.exp(lane_f.astype(F32) * (-2.0 * math.log(ROPE_BASE) / rope))
    cos_v, sin_v = jnp.cos(angles), jnp.sin(angles)
    lane_s = lax.broadcasted_iota(jnp.int32, (batch, batch), 1) % rope
    sin_v = jnp.where(lane_s < rope // 2, -sin_v, sin_v)
    for i in range(heads * rope // batch):
        cos_ref[:, i * batch:(i + 1) * batch] = cos_v
        sin_ref[:, i * batch:(i + 1) * batch] = sin_v
    x_copy().wait()

    def pair_copy(src, dst, i):
        return pltpu.make_async_remote_copy(src_ref=src, dst_ref=dst, send_sem=px_sem.at[0, i], recv_sem=px_sem.at[1, i],
                                            device_id={'tp': mate}, device_id_type=MESH)

    def put_latents(layer, blk, lat):
        q_all[blk, :, pl.ds(0, lora)] = rms(lat[:, :lora], gain_row(qg_ref, layer)).astype(BF16)
        kv = lat[:, lora:]
        q_all[blk, :, pl.ds(lora, latent)] = rms(kv[:, :latent], gain_row(kg_ref, layer)).astype(BF16)
        row0 = pl.multiple_of(blk * rows, rows)
        kr = kv[:, latent:latent + rope]
        kr = jnp.concatenate([kr, kr], axis=1)
        kr = kr * cos_ref[pl.ds(row0, rows), 0:2 * rope] + swap_halves(kr, rope // 2) * sin_ref[pl.ds(row0, rows), 0:2 * rope]
        lane = lax.broadcasted_iota(jnp.int32, kr.shape, 1)
        q_all[blk, :, pl.ds(lora + latent, 2 * rope)] = jnp.where(lane < rope, kr, 0.0).astype(BF16)

    def down_project(layer, blocks, acts, acc):
        def dq_step(i, c):
            slot = lax.rem(i, slots)
            dq_copy(layer, i, slot).wait()
            kv_copy(layer, i, slot).wait()
            a_c = acts(i)
            acc[:, :, 0:lora] += dot_nn(a_c, dq_buf[slot]).reshape(blocks, rows, lora)
            acc[:, :, lora:lora + latent + rope] += dot_nt(a_c, kv_buf[slot]).reshape(blocks, rows, latent + rope)

            @pl.when(i + slots < n_dq)
            def _():
                dq_copy(layer, i + slots, slot).start()
                kv_copy(layer, i + slots, slot).start()
            return c

        lax.fori_loop(0, n_dq, dq_step, 0)

    x_all.wait()
    gain_0 = ag_ref[0:1, :].astype(F32)

    def norm_block(i, c):
        b_all[i] = rms(b_all[i].astype(F32), gain_0).astype(BF16)
        return c

    lax.fori_loop(0, tp_size, norm_block, 0)
    acc_all[...] = jnp.zeros_like(acc_all)
    down_project(0, tp_size, lambda i: b_all[:, :, pl.ds(pl.multiple_of(core * half_k + i * kc, 128), kc)].reshape(batch, kc), acc_all)
    for idx in (0, 1, 2):
        w_copy(0, idx).start()
    start_cache(0)
    w_copy(0, 3).start()
    pl.semaphore_wait(barrier, 4)
    whole = pair_copy(acc_all, acc_rcv, 2)
    whole.start()
    whole.wait_recv()

    def latent_block(i, c):
        put_latents(0, i, acc_all[i] + acc_rcv[i])
        return c

    lax.fori_loop(0, tp_size, latent_block, 0)
    whole.wait_send()

    def front(layer):
        with jax.named_scope('norm'):
            a_buf[...] = rms(xb[...].astype(F32), gain_row(ag_ref, layer)).astype(BF16)
            swap = pair_copy(a_buf.at[:, pl.ds(pl.multiple_of(other * half_k, 128), half_k)], a_pair.at[1], 0)
            swap.start()
            a_pair[0] = a_buf[:, pl.ds(pl.multiple_of(core * half_k, 128), half_k)]
            acc_q[...] = jnp.zeros_like(acc_q)
            swap.wait_recv()
        with jax.named_scope('dq'):
            down_project(layer, 2, lambda i: a_pair[:, :, pl.ds(pl.multiple_of(i * kc, 128), kc)].reshape(2 * rows, kc), acc_q)
        with jax.named_scope('latnorm'):
            back = pair_copy(acc_q.at[1], acc_in, 1)
            back.start()
            back.wait_recv()
            put_latents(layer, me, acc_q[0] + acc_in[...])
            swap.wait_send()
            back.wait_send()
        with jax.named_scope('agq'):
            all_gather(q_all, q_specs, lambda j: None)

    def layer_body(layer, carry):
        more = layer + 1 < layers
        out_c = pltpu.make_async_copy(q_all.at[:, :, pl.ds(lora, latent)], ckv_out.at[layer], out_sem.at[0])
        out_k = pltpu.make_async_copy(q_all.at[:, :, pl.ds(lora + latent, 2 * rope)], kpe_out.at[layer], out_sem.at[1])
        out_c.start()
        out_k.start()

        half_b = batch // 2
        far_rows = pl.ds(pl.multiple_of(other * half_b, half_b), half_b)

        def head_copy(src, dst, i):
            return pltpu.make_async_remote_copy(src_ref=src, dst_ref=dst, send_sem=hx_sem.at[0, i], recv_sem=hx_sem.at[1, i],
                                                device_id={'tp': mate}, device_id_type=MESH)

        w_copy(layer, 0).wait()
        c_q = q_all[:, :, pl.ds(0, lora)].reshape(batch, lora)
        per = nope + rope
        w_n = jnp.concatenate([uq_buf[pl.ds(h * per, nope), :] for h in range(heads)], axis=0)
        w_r = jnp.concatenate([uq_buf[pl.ds(h * per + nope, rope), :] for h in range(heads)], axis=0)
        q_n = dot_nt(c_q, w_n).astype(BF16)
        q_r = dot_nt(c_q, w_r)
        q_r = q_r * cos_ref[...] + swap_halves(q_r, rope // 2) * sin_ref[...]
        lane2 = lax.broadcasted_iota(jnp.int32, (batch, 2 * rope), 1)
        for pair_i in range(heads // 2):
            duo = q_r[:, pair_i * 2 * rope:(pair_i + 1) * 2 * rope]
            swp = pltpu.roll(duo, rope, 1)
            r_buf[2 * pair_i] = jnp.where(lane2 < rope, duo, swp).astype(BF16)
            r_buf[2 * pair_i + 1] = jnp.where(lane2 < rope, swp, duo).astype(BF16)
        head_copy(r_buf.at[:, far_rows], r_in, heads).start()
        w_copy(layer, 1).wait()
        wf[...] = uk_buf[...].astype(F32)
        for h in range(heads):
            wk_h = wf[pl.ds(h, latent, stride=heads), :].astype(BF16)
            u_buf[h] = dot_nt(q_n[:, h * nope:(h + 1) * nope], wk_h).astype(BF16)
            head_copy(u_buf.at[h, far_rows], u_in.at[h], h).start()

        @pl.when(more)
        def _():
            w_copy(layer + 1, 0).start()
            w_copy(layer + 1, 1).start()

        m_rows = 2 * heads * seqs
        own = heads * seqs
        groups = half_b // seqs
        row_b = lax.broadcasted_iota(jnp.int32, (m_rows, keys), 0) % seqs
        lane_k = lax.broadcasted_iota(jnp.int32, (m_rows, keys), 1)
        lane_r = lax.broadcasted_iota(jnp.int32, (m_rows, 2 * rope), 1) // rope

        def att_wait(g):
            slot = lax.rem(g, cslots)
            ckv_copy(layer, g, slot).wait()
            kpe_copy(layer, g, slot).wait()

        def scores(g):
            slot = lax.rem(g, cslots)
            l0 = pl.multiple_of(g * seqs, seqs)
            r0 = pl.multiple_of(core * half_b + g * seqs, seqs)
            blk = core * groups + g
            u_g = jnp.concatenate([u_buf[:, pl.ds(r0, seqs), :].reshape(own, latent),
                                   u_in[:, pl.ds(l0, seqs), :].reshape(own, latent)], axis=0)
            r_g = jnp.concatenate([r_buf[:, pl.ds(r0, seqs), :].reshape(own, 2 * rope),
                                   r_in[:, pl.ds(l0, seqs), :].reshape(own, 2 * rope)], axis=0).astype(F32)
            s_t = dot_nt(u_g, ckv_buf[slot].reshape(seqs * keys, latent))
            s_n = s_t[:, 0:keys]
            for b in range(1, seqs):
                s_n = jnp.where(row_b == b, s_t[:, b * keys:(b + 1) * keys], s_n)
            q_blk = jnp.concatenate(
                [jnp.where(row_b == 2 * b + lane_r, r_g, 0.0).astype(BF16) for b in range(seqs // 2)], axis=1)
            s_r = dot_nn(q_blk, kpe_buf[slot].reshape(seqs * rope, keys))
            cn = tile_rows(q_all[blk, :, pl.ds(lora, latent)].astype(F32), 2 * heads)
            kn = tile_rows(q_all[blk, :, pl.ds(lora + latent, 2 * rope)].astype(F32), 2 * heads)
            fresh = jnp.sum(u_g.astype(F32) * cn, axis=-1, keepdims=True) + jnp.sum(r_g * kn, axis=-1, keepdims=True)
            pos = tile_rows(pos_ref[pl.ds(r0, seqs), :], 2 * heads)
            s = jnp.where(lane_k == pos, fresh, s_n + s_r) * scale
            return jnp.where(lane_k <= pos, s, NEG_INF)

        def context(g, s):
            slot = lax.rem(g, cslots)
            l0 = pl.multiple_of(g * seqs, seqs)
            r0 = pl.multiple_of(core * half_b + g * seqs, seqs)
            blk = core * groups + g
            e = jnp.exp(s - jnp.max(s, axis=-1, keepdims=True))
            prob = (e / jnp.sum(e, axis=-1, keepdims=True)).astype(BF16).astype(F32)
            at_pos = lane_k == tile_rows(pos_ref[pl.ds(r0, seqs), :], 2 * heads)
            p_new = jnp.sum(jnp.where(at_pos, prob, 0.0), axis=-1, keepdims=True)
            p_old = jnp.where(at_pos, 0.0, prob)
            p_blk = jnp.concatenate([jnp.where(row_b == b, p_old, 0.0).astype(BF16) for b in range(seqs)], axis=1)
            cn = tile_rows(q_all[blk, :, pl.ds(lora, latent)].astype(F32), 2 * heads)
            ctx = dot_nn(p_blk, ckv_buf[slot].reshape(seqs * keys, latent)) + p_new * cn
            ctx = ctx.astype(BF16)
            ctx_buf[:, pl.ds(r0, seqs), :] = ctx[:own].reshape(heads, seqs, latent)
            ctx_out[:, pl.ds(l0, seqs), :] = ctx[own:].reshape(heads, seqs, latent)
            ctx_copy(g).start()

        def ctx_copy(g):
            l0 = pl.multiple_of(g * seqs, seqs)
            r0 = pl.multiple_of(core * half_b + g * seqs, seqs)
            return pltpu.make_async_remote_copy(
                src_ref=ctx_out.at[:, pl.ds(l0, seqs)], dst_ref=ctx_buf.at[:, pl.ds(r0, seqs)], send_sem=cx_sem.at[0, g],
                recv_sem=cx_sem.at[1, g], device_id={'tp': mate}, device_id_type=MESH)

        def ctx_arrival(g):
            l0 = pl.multiple_of(g * seqs, seqs)
            r0 = pl.multiple_of(other * half_b + g * seqs, seqs)
            return pltpu.make_async_remote_copy(
                src_ref=ctx_out.at[:, pl.ds(l0, seqs)], dst_ref=ctx_buf.at[:, pl.ds(r0, seqs)], send_sem=cx_sem.at[0, g],
                recv_sem=cx_sem.at[1, g], device_id={'tp': mate}, device_id_type=MESH)

        for h in range(heads):
            head_copy(u_buf.at[h, far_rows], u_in.at[h], h).wait_recv()
        head_copy(r_buf.at[:, far_rows], r_in, heads).wait_recv()
        att_wait(0)
        s_buf[...] = scores(0)

        def att_step(g, c):
            att_wait(g + 1)
            s_now = s_buf[...]
            s_next = scores(g + 1)
            context(g, s_now)
            s_buf[...] = s_next

            @pl.when(g + cslots < groups)
            def _():
                slot = lax.rem(g, cslots)
                ckv_copy(layer, g + cslots, slot).start()
                kpe_copy(layer, g + cslots, slot).start()
            return c

        lax.fori_loop(0, groups - 1, att_step, 0)

        @pl.when(layer == 0)
        def _():
            for idx in (4, 5, 6):
                w_copy(layer, idx).start()

        context(groups - 1, s_buf[...])
        for h in range(heads):
            head_copy(u_buf.at[h, far_rows], u_in.at[h], h).wait_send()
        head_copy(r_buf.at[:, far_rows], r_in, heads).wait_send()
        for g in range(groups):
            ctx_arrival(g).wait_recv()
        for g in range(groups):
            ctx_copy(g).wait_send()

        w_copy(layer, 2).wait()
        wf[...] = uv_buf[...].astype(F32)
        for h in range(heads):
            wv_h = wf[pl.ds(h, latent, stride=heads), :].astype(BF16)
            o_buf[:, h * nope:(h + 1) * nope] = dot_nn(ctx_buf[h], wv_h).astype(BF16)

        @pl.when(more)
        def _():
            w_copy(layer + 1, 2).start()

        w_copy(layer, 3).wait()
        out_c.wait()
        out_k.wait()

        final = reduce_scatter(lambda j: dot_nn(o_buf[...], wo_buf[:, pl.ds(j * cw, cw)]))

        @pl.when(more)
        def _():
            start_dq(layer + 1)
            start_cache(layer + 1)
            w_copy(layer + 1, 3).start()

        rs_drain(final)

        b_all[me] = rms(xb[...].astype(F32), gain_row(mg_ref, layer)).astype(BF16)
        w_copy(layer, 4).wait()
        w_copy(layer, 5).wait()

        def gate_up(j):
            cols = pl.ds(j * gw, gw)
            b_c = b_all[:, :, cols].reshape(batch, gw)
            val = dot_nt(b_c, wgu_buf[:, cols])
            if j == 0:
                gu_acc[...] = val
            else:
                gu_acc[...] += val

        all_gather(b_all, b_specs, gate_up)
        gate = gu_acc[:, 0:ffn]
        act_buf[...] = (gate * lax.logistic(gate) * gu_acc[:, ffn:2 * ffn]).astype(BF16)
        w_copy(layer, 6).wait()

        @pl.when(more)
        def _():
            w_copy(layer + 1, 4).start()
            w_copy(layer + 1, 5).start()

        final2 = reduce_scatter(lambda j: dot_nn(act_buf[...], wd_buf[:, pl.ds(j * cw, cw)]))

        @pl.when(more)
        def _():
            w_copy(layer + 1, 6).start()

        def send_rows(j):
            @pl.when(jnp.logical_not(more))
            def _():
                b_all[me, :, pl.ds(j * cw, cw)] = xb[:, pl.ds(j * cw, cw)]
                ag_first(b_all, j, x_specs[j])

        rs_drain(final2, send_rows)

        @pl.when(more)
        def _():
            front(layer + 1)
        return carry

    lax.fori_loop(0, layers, layer_body, 0)

    def put(j):
        cols = pl.ds(j * cw, cw)
        pltpu.make_async_copy(b_all.at[:, :, cols], x_out.at[:, :, cols], out_sem.at[j]).start()

    all_gather(b_all, x_specs, put, started=True)
    for j in range(chunks):
        cols = pl.ds(j * cw, cw)
        pltpu.make_async_copy(b_all.at[:, :, cols], x_out.at[:, :, cols], out_sem.at[j]).wait()


def solution(mesh):
    tp = mesh.shape['tp']
    cache_spec = P(None, 'dp', None, None)
    head_spec = P(None, None, 'tp', None)
    weight_specs = (P(), P(), P(), P(), P(), head_spec, head_spec, head_spec, P(None, 'tp', None, None), P(), P(None, None, 'tp'), P(None, None, 'tp'), P(None, 'tp', None))
    in_specs = (P('dp', None), P('dp'), cache_spec, cache_spec) + weight_specs
    out_specs = (P('dp', None), P(None, 'dp', None), P(None, 'dp', None))

    def device_body(x_in, pos_ids, ckv_cache, kpe_cache, attn_gain, w_dq, q_gain, w_dkv, kv_gain, w_uq, w_uk, w_uv, w_o,
                    mlp_gain, w_gate, w_up, w_down):
        batch, model = x_in.shape
        layers, _, keys, latent = ckv_cache.shape
        rope = kpe_cache.shape[-1]
        lora = w_dq.shape[-1]
        heads, per = w_uq.shape[2:]
        nope = w_uk.shape[-1]
        ffn = w_gate.shape[-1]
        rows = batch // tp
        kc, slots, chunks, gchunks, direct, seqs, cslots = 512, 3, 4, 4, 1, rows, 3
        hb = pl.BlockSpec(memory_space=pl.ANY)
        dma = pltpu.SemaphoreType.DMA
        qw = lora + latent + 2 * rope
        ch = model // chunks // 2
        scratch = [
            pltpu.VMEM((1, batch), jnp.int32),
            pltpu.VMEM((layers, model), BF16),
            pltpu.VMEM((layers, model), BF16),
            pltpu.VMEM((layers, lora), BF16),
            pltpu.VMEM((layers, latent), BF16),
            pltpu.VMEM((batch, heads * rope), F32),
            pltpu.VMEM((batch, heads * rope), F32),
            pltpu.VMEM((batch, keys), jnp.int32),
            pltpu.VMEM((rows, model), BF16),
            pltpu.VMEM((rows, model), BF16),
            pltpu.VMEM((2, rows, model // 2), BF16),
            pltpu.VMEM((rows, lora + latent + 2 * rope), F32),
            pltpu.VMEM((tp, rows, model), BF16),
            pltpu.VMEM((tp, rows, qw), BF16),
            pltpu.VMEM((2, rows, lora + latent + 2 * rope), F32),
            pltpu.VMEM((tp, rows, lora + latent + 2 * rope), F32),
            pltpu.VMEM((tp, rows, lora + latent + 2 * rope), F32),
            pltpu.VMEM((heads, batch, latent), BF16),
            pltpu.VMEM((heads, batch, 2 * rope), BF16),
            pltpu.VMEM((heads, batch // 2, latent), BF16),
            pltpu.VMEM((heads, batch // 2, 2 * rope), BF16),
            pltpu.VMEM((heads, batch, latent), BF16),
            pltpu.VMEM((heads, batch // 2, latent), BF16),
            pltpu.VMEM((batch, heads * nope), BF16),
            pltpu.VMEM((latent * heads, nope), F32),
            pltpu.VMEM((batch, 2 * ffn), F32),
            pltpu.VMEM((batch, ffn), BF16),
            pltpu.VMEM((tp // 2, 2, rows, model), BF16),
            pltpu.VMEM((tp // 2, rows, model), BF16),
            pltpu.VMEM((tp // 2, rows, model), BF16),
            pltpu.VMEM((2, rows, model // 2), BF16),
            pltpu.VMEM((2, rows, model // 2), BF16),
            pltpu.VMEM((2, rows, model), BF16),
            pltpu.VMEM((slots, kc, lora), BF16),
            pltpu.VMEM((slots, latent + rope, kc), BF16),
            pltpu.VMEM((heads * per, lora), BF16),
            pltpu.VMEM((latent * heads, nope), BF16),
            pltpu.VMEM((latent * heads, nope), BF16),
            pltpu.VMEM((heads * nope, model), BF16),
            pltpu.VMEM((2 * ffn, model), BF16),
            pltpu.VMEM((ffn, model), BF16),
            pltpu.VMEM((cslots, seqs, keys, latent), BF16),
            pltpu.VMEM((cslots, seqs, rope, keys), BF16),
            pltpu.VMEM((2 * heads * seqs, keys), F32),
            dma((2,)), dma((5,)), dma((2, 3)), dma((2, heads + 1)), dma((2, batch // 2 // seqs)), dma((slots,)), dma((slots,)), dma((7,)), dma((2, cslots)), dma((gchunks,)),
            dma((gchunks, 9)), dma((gchunks, 9)), dma((chunks, 7)), dma((chunks, 7)),
        ]
        cfg = dict(tp=tp, layers=layers, heads=heads, kc=kc, slots=slots, chunks=chunks, seqs=seqs, cslots=cslots, gchunks=gchunks, direct=direct)
        call = pl.pallas_call(
            functools.partial(step_kernel, cfg),
            out_shape=(jax.ShapeDtypeStruct((tp, rows, model), BF16),
                       jax.ShapeDtypeStruct((layers, tp, rows, latent), BF16),
                       jax.ShapeDtypeStruct((layers, tp, rows, 2 * rope), BF16)),
            in_specs=[hb] * 17,
            out_specs=(hb, hb, hb),
            scratch_shapes=scratch,
            compiler_params=pltpu.CompilerParams(collective_id=0, has_side_effects=True, vmem_limit_bytes=67043328),
            name='decode_step',
        )
        x_o, c_o, k_o = call(
            x_in.reshape(tp, rows, model), pos_ids.reshape(1, batch), attn_gain, mlp_gain, q_gain, kv_gain,
            w_dq, w_dkv.transpose(0, 2, 1), w_uq.transpose(0, 2, 3, 1).reshape(layers, heads * per, lora),
            w_uk.reshape(layers, latent * heads, nope), w_uv.reshape(layers, latent * heads, nope),
            w_o.reshape(layers, heads * nope, model),
            w_gate.transpose(0, 2, 1), w_up.transpose(0, 2, 1), w_down,
            ckv_cache, kpe_cache.transpose(0, 1, 3, 2))
        return (x_o.reshape(batch, model), c_o.reshape(layers, batch, latent),
                k_o.reshape(layers, batch, 2 * rope)[..., :rope])

    return jax.shard_map(device_body, mesh=mesh, in_specs=in_specs, out_specs=out_specs, check_vma=False)
```

```python
import math
import functools
import jax
import jax.numpy as jnp
from jax import lax
from jax.experimental import pallas as pl
from jax.experimental.pallas import tpu as pltpu
from jax.sharding import PartitionSpec as P

NORM_EPS = 1e-6
ROPE_BASE = 10000.0
F32 = jnp.float32
BF16 = jnp.bfloat16
MESH = pl.DeviceIdType.MESH
NEG_INF = float('-inf')


def rms(values, gain):
    inv = lax.rsqrt(jnp.mean(values * values, axis=-1, keepdims=True) + NORM_EPS)
    return values * inv * gain


def dot_nt(lhs, rhs):
    return lax.dot_general(lhs, rhs, (((1,), (1,)), ((), ())), preferred_element_type=F32)


def dot_nn(lhs, rhs):
    return jnp.dot(lhs, rhs, preferred_element_type=F32)


def swap_halves(values, half):
    width = values.shape[-1]
    lane = lax.broadcasted_iota(jnp.int32, values.shape, 1)
    up = pltpu.roll(values, half, 1)
    down = pltpu.roll(values, width - half, 1)
    return jnp.where(lane % (2 * half) < half, down, up)


def tile_rows(values, count):
    return jnp.concatenate([values] * count, axis=0)


def step_kernel(cfg, x_hbm, pos_hbm, ag_hbm, mg_hbm, qg_hbm, kg_hbm,
                wdq, wkv, wuq, wuk, wuv, wo, wg, wu, wd, ckv_hbm, kpe_hbm,
                x_out, ckv_out, kpe_out,
                pos_row, ag_ref, mg_ref, qg_ref, kg_ref, cos_ref, sin_ref, pos_ref,
                xb, a_buf, a_pair, b_all, q_all, acc_all, acc_rcv, u_buf, r_buf, u_in, r_in, ctx_buf, ctx_out, o_buf, wf,
                act_buf,
                part, d2d, rel, cmb, fin,
                dq_buf, kv_buf, uq_buf, uk_buf, uv_buf, wo_buf, wgu_buf, wd_buf, ckv_buf, kpe_buf, s_buf, kt_buf,
                x_sem, s_sem, px_sem, hx_sem, cx_sem, dq_sem, kv_sem, w_sem, c_sem, out_sem,
                ag_send, ag_recv, rs_send, rs_recv):
    tp_size, layers, heads, kc, slots, seqs = (
        cfg['tp'], cfg['layers'], cfg['heads'], cfg['kc'], cfg['slots'], cfg['seqs'])
    nchip = tp_size // 2
    model = xb.shape[1]
    rows = xb.shape[0]
    lora = uq_buf.shape[1]
    latent = ckv_buf.shape[-1]
    rope = kpe_buf.shape[2]
    nope = uk_buf.shape[1]
    keys = ckv_buf.shape[2]
    batch = rows * tp_size
    ffn = wd_buf.shape[0]
    cslots = cfg['cslots']
    half_k = model // 2
    n_dq = half_k // kc
    widths = cfg['widths']
    chunks = len(widths)
    offs = [sum(widths[:j]) for j in range(chunks)]
    scale = float((nope + rope) ** -0.5)

    psum = d2d
    gu_acc = acc_all.at[:, :, 0:2 * wd_buf.shape[0]]
    acc_q, acc_in = acc_all.at[0:2], acc_rcv.at[0]
    me = lax.axis_index('tp')
    core = lax.rem(me, 2)
    chip = me // 2
    other = 1 - core
    rchip = lax.rem(chip + 1, nchip)
    lchip = lax.rem(chip + nchip - 1, nchip)
    ochip = lax.rem(chip + 2, nchip)
    mate = 2 * chip + other
    right = 2 * rchip + core
    left = 2 * lchip + core
    opp = 2 * ochip + core

    barrier = pltpu.get_barrier_semaphore()
    for peer in (mate, right, left, opp):
        pl.semaphore_signal(barrier, inc=1, device_id={'tp': peer}, device_id_type=MESH)

    def x_copy():
        return pltpu.make_async_copy(x_hbm.at[me], xb, x_sem.at[0])

    def dq_copy(layer, i, slot):
        off = pl.multiple_of(core * half_k + i * kc, 128)
        return pltpu.make_async_copy(wdq.at[layer, pl.ds(off, kc), :], dq_buf.at[slot], dq_sem.at[slot])

    def kv_copy(layer, i, slot):
        off = pl.multiple_of(core * half_k + i * kc, 128)
        return pltpu.make_async_copy(wkv.at[layer, :, pl.ds(off, kc)], kv_buf.at[slot], kv_sem.at[slot])

    weights = [(wuq, uq_buf), (wuk, uk_buf), (wuv, uv_buf), (wo, wo_buf), (wg, wgu_buf.at[0:ffn]), (wu, wgu_buf.at[ffn:2 * ffn]), (wd, wd_buf)]

    def w_copy(layer, idx):
        src, dst = weights[idx]
        return pltpu.make_async_copy(src.at[layer], dst, w_sem.at[idx])

    def ckv_copy(layer, g, slot):
        return pltpu.make_async_copy(ckv_hbm.at[layer, pl.ds(core * (batch // 2) + g * seqs, seqs)], ckv_buf.at[slot], c_sem.at[0, slot])

    def kpe_copy(layer, g, slot):
        return pltpu.make_async_copy(kpe_hbm.at[layer, pl.ds(core * (batch // 2) + g * seqs, seqs)], kpe_buf.at[slot], c_sem.at[1, slot])

    def start_dq(layer):
        for s in range(slots):
            dq_copy(layer, s, s).start()
            kv_copy(layer, s, s).start()

    def start_cache(layer):
        for s in range(cslots):
            ckv_copy(layer, s, s).start()
            kpe_copy(layer, s, s).start()

    def remote(src, dst, sems, recvs, j, kind, dev):
        return pltpu.make_async_remote_copy(src_ref=src, dst_ref=dst, send_sem=sems.at[j, kind],
                                            recv_sem=recvs.at[j, kind], device_id={'tp': dev}, device_id_type=MESH)

    def ag_desc(buf, j, spec, kind, blk, dev):
        off, half_a, width, direct = spec
        lo, size = off, width
        if not direct and kind in (3, 7):
            size = half_a
        elif not direct and kind in (4, 8):
            lo, size = off + half_a, width - half_a
        ref = buf.at[blk, :, pl.ds(lo, size)]
        return remote(ref, ref, ag_send, ag_recv, j, kind, dev)

    mleft = 2 * lchip + other
    mright = 2 * rchip + other
    mopp = 2 * ochip + other
    ag_out = [(me, mate), (me, right), (me, left), (left, right), (right, left), (left, mate), (right, mate), (opp, mate), (opp, mate)]
    ag_in = [mate, left, right, opp, opp, mleft, mright, mopp, mopp]

    def ag_route(spec, kind):
        if kind == 3 and spec[3]:
            return me, opp
        return ag_out[kind]

    def ag_start(buf, j, spec, kind):
        ag_desc(buf, j, spec, kind, *ag_route(spec, kind)).start()

    def ag_wait(buf, j, spec, kind):
        ag_desc(buf, j, spec, kind, ag_in[kind], mate).wait_recv()

    def ag_first(buf, j, spec):
        for kind in ((1, 2, 3, 0) if spec[3] else (1, 2, 0)):
            ag_start(buf, j, spec, kind)

    def all_gather(buf, specs, consume, started=False):
        n = len(specs)
        for j in range(n):
            if not started:
                ag_first(buf, j, specs[j])

        def forward(j):
            direct = specs[j][3]
            for kind in (1, 2):
                ag_wait(buf, j, specs[j], kind)
                if not direct:
                    ag_start(buf, j, specs[j], kind + 2)
                ag_start(buf, j, specs[j], kind + 4)

        def pass_far(j):
            for kind in ((3,) if specs[j][3] else (3, 4)):
                ag_wait(buf, j, specs[j], kind)
                ag_start(buf, j, specs[j], kind + 4)

        def finish(j):
            for kind in ((0, 5, 6, 7) if specs[j][3] else (0, 5, 6, 7, 8)):
                ag_wait(buf, j, specs[j], kind)
            with jax.named_scope('consume'):
                consume(j)

        lead = sum(spec[3] for spec in specs)
        if n == 1:
            lead = 0
        for j in range(n):
            forward(j)
            if 1 <= j <= lead:
                pass_far(j - 1)
        for j in range(lead):
            finish(j)
        pass_far(lead)
        for j in range(lead, n):
            if j + 1 < n:
                pass_far(j + 1)
            finish(j)
        for j in range(n):
            for kind in range(9):
                if not (specs[j][3] and kind in (4, 8)):
                    ag_desc(buf, j, specs[j], kind, *ag_route(specs[j], kind)).wait_send()

    def rs_desc(j, kind):
        o, w = offs[j], widths[j]
        h = w // 2
        ca, cb = pl.ds(o, h), pl.ds(o + h, h)
        hj = pl.ds(o // 2, h)
        full = pl.ds(o, w)
        src, dst, dev = [
            lambda: (part.at[:, other, :, full], d2d.at[:, :, full], mate),
            lambda: (psum.at[ochip, :, ca], rel.at[0, :, hj], right),
            lambda: (psum.at[ochip, :, cb], rel.at[1, :, hj], left),
            lambda: (psum.at[rchip, :, cb], fin.at[0, :, cb], right),
            lambda: (psum.at[lchip, :, ca], fin.at[1, :, ca], left),
            lambda: (cmb.at[0, :, hj], fin.at[0, :, ca], right),
            lambda: (cmb.at[1, :, hj], fin.at[1, :, cb], left),
        ][kind]()
        return remote(src, dst, rs_send, rs_recv, j, kind, dev)

    def reduce_scatter(product):
        def mm(j):
            o, w = offs[j], widths[j]
            part[:, :, :, pl.ds(o, w)] = product(pl.ds(o, w)).reshape(nchip, 2, rows, w).astype(BF16)
            rs_desc(j, 0).start()

        def pair(j):
            rs_desc(j, 0).wait_recv()
            cols = pl.ds(offs[j], widths[j])
            psum[ochip, :, cols] = (part[ochip, core, :, cols].astype(F32) + d2d[ochip, :, cols].astype(F32)).astype(BF16)
            rs_desc(j, 1).start()
            rs_desc(j, 2).start()
            for cc in (rchip, lchip, chip):
                psum[cc, :, cols] = (part[cc, core, :, cols].astype(F32) + d2d[cc, :, cols].astype(F32)).astype(BF16)

        def combine(j):
            o, h = offs[j], widths[j] // 2
            hj = pl.ds(o // 2, h)
            rs_desc(j, 1).wait_recv()
            cmb[0, :, hj] = (psum[rchip, :, pl.ds(o, h)].astype(F32) + rel[0, :, hj].astype(F32)).astype(BF16)
            rs_desc(j, 5).start()
            rs_desc(j, 2).wait_recv()
            cmb[1, :, hj] = (psum[lchip, :, pl.ds(o + h, h)].astype(F32) + rel[1, :, hj].astype(F32)).astype(BF16)
            rs_desc(j, 6).start()

        def final(j):
            for kind in (3, 4, 5, 6):
                rs_desc(j, kind).wait_recv()
            cols = pl.ds(offs[j], widths[j])
            total = psum[chip, :, cols].astype(F32) + fin[0, :, cols].astype(F32) + fin[1, :, cols].astype(F32)
            xb[:, cols] = (xb[:, cols].astype(F32) + total).astype(BF16)

        for j in range(chunks + 1):
            if j < chunks:
                mm(j)
            if j > 0:
                pair(j - 1)
        for j in range(chunks):
            rs_desc(j, 3).start()
            rs_desc(j, 4).start()
        for j in range(chunks):
            combine(j)
        return final

    def rs_drain(final, hook=None):
        for j in range(chunks):
            final(j)
            if hook is not None:
                hook(j)
        for j in range(chunks):
            for kind in range(7):
                rs_desc(j, kind).wait_send()

    gchunks = cfg['gchunks']
    gw = model // gchunks
    gh = (gw // 128 + 1) // 2 * 128
    b_specs = [(j * gw, gh, gw, j < cfg['direct']) for j in range(gchunks)]
    x_specs = [(offs[j], widths[j] // 2, widths[j], False) for j in range(chunks)]
    qw = q_all.shape[2]
    q_specs = [(0, 0, qw, True)]

    def gain_row(ref, layer):
        vals = ref[...].astype(F32)
        row = vals[0:1]
        for i in range(1, layers):
            row = jnp.where(layer == i, vals[i:i + 1], row)
        return row

    small = [(pos_hbm, pos_row), (ag_hbm, ag_ref), (mg_hbm, mg_ref), (qg_hbm, qg_ref), (kg_hbm, kg_ref)]
    x_all = pltpu.make_async_copy(x_hbm, b_all, x_sem.at[1])
    x_all.start()
    x_copy().start()
    for i, (src, dst) in enumerate(small):
        pltpu.make_async_copy(src, dst, s_sem.at[i]).start()
    def pair_copy(src, dst, i):
        return pltpu.make_async_remote_copy(src_ref=src, dst_ref=dst, send_sem=px_sem.at[0, i], recv_sem=px_sem.at[1, i],
                                            device_id={'tp': mate}, device_id_type=MESH)

    def put_latents(layer, blk, lat):
        q_all[blk, :, pl.ds(0, lora)] = rms(lat[:, :lora], gain_row(qg_ref, layer)).astype(BF16)
        kv = lat[:, lora:]
        q_all[blk, :, pl.ds(lora, latent)] = rms(kv[:, :latent], gain_row(kg_ref, layer)).astype(BF16)
        row0 = pl.multiple_of(blk * rows, rows)
        kr = kv[:, latent:latent + rope]
        kr = jnp.concatenate([kr, kr], axis=1)
        kr = kr * cos_ref[pl.ds(row0, rows), 0:2 * rope] + swap_halves(kr, rope // 2) * sin_ref[pl.ds(row0, rows), 0:2 * rope]
        lane = lax.broadcasted_iota(jnp.int32, kr.shape, 1)
        q_all[blk, :, pl.ds(lora + latent, 2 * rope)] = jnp.where(lane < rope, kr, 0.0).astype(BF16)

    def down_project(layer, blocks, acts, acc):
        def dq_step(i, c):
            slot = lax.rem(i, slots)
            dq_copy(layer, i, slot).wait()
            kv_copy(layer, i, slot).wait()
            a_c = acts(i)
            acc[:, :, 0:lora] += dot_nn(a_c, dq_buf[slot]).reshape(blocks, rows, lora)
            acc[:, :, lora:lora + latent + rope] += dot_nt(a_c, kv_buf[slot]).reshape(blocks, rows, latent + rope)

            @pl.when(i + slots < n_dq)
            def _():
                dq_copy(layer, i + slots, slot).start()
                kv_copy(layer, i + slots, slot).start()
            return c

        lax.fori_loop(0, n_dq, dq_step, 0)

    acc_all[...] = jnp.zeros_like(acc_all)
    for i, (src, dst) in enumerate(small):
        pltpu.make_async_copy(src, dst, s_sem.at[i]).wait()
    x_all.wait()
    start_dq(0)
    x_copy().wait()
    my_half = pl.ds(pl.multiple_of(core * half_k, 128), half_k)
    gain_0 = ag_ref[0:1, :].astype(F32)
    gain_h = jnp.where(core == 0, gain_0[:, :half_k], gain_0[:, half_k:])

    def norm_block(i, c):
        vals = b_all[i].astype(F32)
        inv = lax.rsqrt(jnp.mean(vals * vals, axis=-1, keepdims=True) + NORM_EPS)
        b_all[i, :, my_half] = (b_all[i, :, my_half].astype(F32) * inv * gain_h).astype(BF16)
        return c

    lax.fori_loop(0, tp_size, norm_block, 0)
    down_project(0, tp_size, lambda i: b_all[:, :, pl.ds(pl.multiple_of(core * half_k + i * kc, 128), kc)].reshape(batch, kc), acc_all)
    for idx in (0, 1, 2):
        w_copy(0, idx).start()
    start_cache(0)
    w_copy(0, 3).start()
    pl.semaphore_wait(barrier, 4)
    pieces = 4
    per_piece = tp_size // pieces

    def piece(i):
        blks = pl.ds(i * per_piece, per_piece)
        return pair_copy(acc_all.at[blks], acc_rcv.at[blks], 2 + i)

    for i in range(pieces):
        piece(i).start()
    pos_f = jnp.transpose(jnp.broadcast_to(pos_row[...].astype(F32), (batch, batch)))
    pos_ref[...] = pos_f.astype(jnp.int32)
    lane_f = lax.broadcasted_iota(jnp.int32, (batch, batch), 1) % (rope // 2)
    angles = pos_f * jnp.exp(lane_f.astype(F32) * (-2.0 * math.log(ROPE_BASE) / rope))
    cos_v, sin_v = jnp.cos(angles), jnp.sin(angles)
    lane_s = lax.broadcasted_iota(jnp.int32, (batch, batch), 1) % rope
    sin_v = jnp.where(lane_s < rope // 2, -sin_v, sin_v)
    for i in range(heads * rope // batch):
        cos_ref[:, i * batch:(i + 1) * batch] = cos_v
        sin_ref[:, i * batch:(i + 1) * batch] = sin_v

    def latent_block(i, c):
        put_latents(0, i, acc_all[i] + acc_rcv[i])
        return c

    for i in range(pieces):
        piece(i).wait_recv()
        lax.fori_loop(i * per_piece, (i + 1) * per_piece, latent_block, 0)
    for i in range(pieces):
        piece(i).wait_send()

    def front(layer):
        with jax.named_scope('norm'):
            a_buf[...] = rms(xb[...].astype(F32), gain_row(ag_ref, layer)).astype(BF16)
            swap = pair_copy(a_buf.at[:, pl.ds(pl.multiple_of(other * half_k, 128), half_k)], a_pair.at[1], 0)
            swap.start()
            a_pair[0] = a_buf[:, pl.ds(pl.multiple_of(core * half_k, 128), half_k)]
            acc_q[...] = jnp.zeros(acc_q.shape, F32)
            swap.wait_recv()
        with jax.named_scope('dq'):
            down_project(layer, 2, lambda i: a_pair[:, :, pl.ds(pl.multiple_of(i * kc, 128), kc)].reshape(2 * rows, kc), acc_q)
        with jax.named_scope('latnorm'):
            back = pair_copy(acc_q.at[1], acc_in, 1)
            back.start()
            back.wait_recv()
            put_latents(layer, me, acc_q[0] + acc_in[...])
            swap.wait_send()
            back.wait_send()
        with jax.named_scope('agq'):
            all_gather(q_all, q_specs, lambda j: None)

    def layer_body(layer, carry):
        more = layer + 1 < layers
        out_c = pltpu.make_async_copy(q_all.at[:, :, pl.ds(lora, latent)], ckv_out.at[layer], out_sem.at[0])
        kpe_t = jnp.transpose(q_all[:, :, pl.ds(lora + latent, 2 * rope)].astype(F32).reshape(batch, 2 * rope))
        kt_buf[...] = kpe_t[0:rope].astype(BF16)
        out_k = pltpu.make_async_copy(kt_buf, kpe_out.at[layer], out_sem.at[1])
        out_c.start()
        out_k.start()

        half_b = batch // 2
        far_rows = pl.ds(pl.multiple_of(other * half_b, half_b), half_b)

        def head_copy(src, dst, i):
            return pltpu.make_async_remote_copy(src_ref=src, dst_ref=dst, send_sem=hx_sem.at[0, i], recv_sem=hx_sem.at[1, i],
                                                device_id={'tp': mate}, device_id_type=MESH)

        w_copy(layer, 0).wait()
        c_q = q_all[:, :, pl.ds(0, lora)].reshape(batch, lora)
        per = nope + rope
        w_n = jnp.concatenate([uq_buf[pl.ds(h * per, nope), :] for h in range(heads)], axis=0)
        w_r = jnp.concatenate([uq_buf[pl.ds(h * per + nope, rope), :] for h in range(heads)], axis=0)
        q_n = dot_nt(c_q, w_n).astype(BF16)
        q_r = dot_nt(c_q, w_r)
        q_r = q_r * cos_ref[...] + swap_halves(q_r, rope // 2) * sin_ref[...]
        lane2 = lax.broadcasted_iota(jnp.int32, (batch, 2 * rope), 1)
        for pair_i in range(heads // 2):
            duo = q_r[:, pair_i * 2 * rope:(pair_i + 1) * 2 * rope]
            swp = pltpu.roll(duo, rope, 1)
            r_buf[2 * pair_i] = jnp.where(lane2 < rope, duo, swp).astype(BF16)
            r_buf[2 * pair_i + 1] = jnp.where(lane2 < rope, swp, duo).astype(BF16)
        head_copy(r_buf.at[:, far_rows], r_in, heads).start()
        w_copy(layer, 1).wait()
        wf[...] = uk_buf[...].astype(F32)
        for h in range(heads):
            wk_h = wf[pl.ds(h, latent, stride=heads), :].astype(BF16)
            u_buf[h] = dot_nt(q_n[:, h * nope:(h + 1) * nope], wk_h).astype(BF16)
            head_copy(u_buf.at[h, far_rows], u_in.at[h], h).start()

        @pl.when(more)
        def _():
            w_copy(layer + 1, 0).start()
            w_copy(layer + 1, 1).start()

        m_rows = 2 * heads * seqs
        own = heads * seqs
        groups = half_b // seqs
        row_b = lax.broadcasted_iota(jnp.int32, (m_rows, keys), 0) % seqs
        lane_k = lax.broadcasted_iota(jnp.int32, (m_rows, keys), 1)
        lane_r = lax.broadcasted_iota(jnp.int32, (m_rows, 2 * rope), 1) // rope

        def att_wait(g):
            slot = lax.rem(g, cslots)
            ckv_copy(layer, g, slot).wait()
            kpe_copy(layer, g, slot).wait()

        def scores(g):
            slot = lax.rem(g, cslots)
            l0 = pl.multiple_of(g * seqs, seqs)
            r0 = pl.multiple_of(core * half_b + g * seqs, seqs)
            blk = core * groups + g
            u_g = jnp.concatenate([u_buf[:, pl.ds(r0, seqs), :].reshape(own, latent),
                                   u_in[:, pl.ds(l0, seqs), :].reshape(own, latent)], axis=0)
            r_g = jnp.concatenate([r_buf[:, pl.ds(r0, seqs), :].reshape(own, 2 * rope),
                                   r_in[:, pl.ds(l0, seqs), :].reshape(own, 2 * rope)], axis=0).astype(F32)
            s_t = dot_nt(u_g, ckv_buf[slot].reshape(seqs * keys, latent))
            s_n = s_t[:, 0:keys]
            for b in range(1, seqs):
                s_n = jnp.where(row_b == b, s_t[:, b * keys:(b + 1) * keys], s_n)
            q_blk = jnp.concatenate(
                [jnp.where(row_b == 2 * b + lane_r, r_g, 0.0).astype(BF16) for b in range(seqs // 2)], axis=1)
            s_r = dot_nn(q_blk, kpe_buf[slot].reshape(seqs * rope, keys))
            cn = tile_rows(q_all[blk, :, pl.ds(lora, latent)].astype(F32), 2 * heads)
            kn = tile_rows(q_all[blk, :, pl.ds(lora + latent, 2 * rope)].astype(F32), 2 * heads)
            fresh = jnp.sum(u_g.astype(F32) * cn, axis=-1, keepdims=True) + jnp.sum(r_g * kn, axis=-1, keepdims=True)
            pos = tile_rows(pos_ref[pl.ds(r0, seqs), :], 2 * heads)
            s = jnp.where(lane_k == pos, fresh, s_n + s_r) * scale
            return jnp.where(lane_k <= pos, s, NEG_INF)

        def context(g, s):
            slot = lax.rem(g, cslots)
            l0 = pl.multiple_of(g * seqs, seqs)
            r0 = pl.multiple_of(core * half_b + g * seqs, seqs)
            blk = core * groups + g
            e = jnp.exp(s - jnp.max(s, axis=-1, keepdims=True))
            prob = (e / jnp.sum(e, axis=-1, keepdims=True)).astype(BF16).astype(F32)
            at_pos = lane_k == tile_rows(pos_ref[pl.ds(r0, seqs), :], 2 * heads)
            p_new = jnp.sum(jnp.where(at_pos, prob, 0.0), axis=-1, keepdims=True)
            p_old = jnp.where(at_pos, 0.0, prob)
            p_blk = jnp.concatenate([jnp.where(row_b == b, p_old, 0.0).astype(BF16) for b in range(seqs)], axis=1)
            cn = tile_rows(q_all[blk, :, pl.ds(lora, latent)].astype(F32), 2 * heads)
            ctx = dot_nn(p_blk, ckv_buf[slot].reshape(seqs * keys, latent)) + p_new * cn
            ctx = ctx.astype(BF16)
            ctx_buf[:, pl.ds(r0, seqs), :] = ctx[:own].reshape(heads, seqs, latent)
            ctx_out[:, pl.ds(l0, seqs), :] = ctx[own:].reshape(heads, seqs, latent)
            ctx_copy(g).start()

        def ctx_copy(g):
            l0 = pl.multiple_of(g * seqs, seqs)
            r0 = pl.multiple_of(core * half_b + g * seqs, seqs)
            return pltpu.make_async_remote_copy(
                src_ref=ctx_out.at[:, pl.ds(l0, seqs)], dst_ref=ctx_buf.at[:, pl.ds(r0, seqs)], send_sem=cx_sem.at[0, g],
                recv_sem=cx_sem.at[1, g], device_id={'tp': mate}, device_id_type=MESH)

        def ctx_arrival(g):
            l0 = pl.multiple_of(g * seqs, seqs)
            r0 = pl.multiple_of(other * half_b + g * seqs, seqs)
            return pltpu.make_async_remote_copy(
                src_ref=ctx_out.at[:, pl.ds(l0, seqs)], dst_ref=ctx_buf.at[:, pl.ds(r0, seqs)], send_sem=cx_sem.at[0, g],
                recv_sem=cx_sem.at[1, g], device_id={'tp': mate}, device_id_type=MESH)

        for h in range(heads):
            head_copy(u_buf.at[h, far_rows], u_in.at[h], h).wait_recv()
        head_copy(r_buf.at[:, far_rows], r_in, heads).wait_recv()
        att_wait(0)
        s_buf[...] = scores(0)

        def att_step(g, c):
            att_wait(g + 1)
            s_now = s_buf[...]
            s_next = scores(g + 1)
            context(g, s_now)
            s_buf[...] = s_next
            return c

        lax.fori_loop(0, groups - 1, att_step, 0)

        @pl.when(layer == 0)
        def _():
            for idx in (4, 5, 6):
                w_copy(layer, idx).start()

        context(groups - 1, s_buf[...])
        for h in range(heads):
            head_copy(u_buf.at[h, far_rows], u_in.at[h], h).wait_send()
        head_copy(r_buf.at[:, far_rows], r_in, heads).wait_send()
        w_copy(layer, 2).wait()
        wf[...] = uv_buf[...].astype(F32)
        for g in range(groups):
            ctx_arrival(g).wait_recv()
        for g in range(groups):
            ctx_copy(g).wait_send()
        for h in range(heads):
            wv_h = wf[pl.ds(h, latent, stride=heads), :].astype(BF16)
            o_buf[:, h * nope:(h + 1) * nope] = dot_nn(ctx_buf[h], wv_h).astype(BF16)

        @pl.when(more)
        def _():
            w_copy(layer + 1, 2).start()

        w_copy(layer, 3).wait()
        out_c.wait()
        out_k.wait()

        final = reduce_scatter(lambda cols: dot_nn(o_buf[...], wo_buf[:, cols]))

        @pl.when(more)
        def _():
            start_dq(layer + 1)
            start_cache(layer + 1)
            w_copy(layer + 1, 3).start()

        rs_drain(final)

        b_all[me] = rms(xb[...].astype(F32), gain_row(mg_ref, layer)).astype(BF16)
        w_copy(layer, 4).wait()
        w_copy(layer, 5).wait()

        def gate_up(j):
            cols = pl.ds(j * gw, gw)
            b_c = b_all[:, :, cols].reshape(batch, gw)
            val = dot_nt(b_c, wgu_buf[:, cols]).reshape(tp_size, rows, 2 * ffn)
            if j == 0:
                gu_acc[...] = val
            else:
                gu_acc[...] += val

        all_gather(b_all, b_specs, gate_up)
        both = gu_acc[...].reshape(batch, 2 * ffn)
        gate = both[:, 0:ffn]
        act_buf[...] = (gate * lax.logistic(gate) * both[:, ffn:2 * ffn]).astype(BF16)
        w_copy(layer, 6).wait()

        @pl.when(more)
        def _():
            w_copy(layer + 1, 4).start()
            w_copy(layer + 1, 5).start()

        final2 = reduce_scatter(lambda cols: dot_nn(act_buf[...], wd_buf[:, cols]))

        @pl.when(more)
        def _():
            w_copy(layer + 1, 6).start()

        def send_rows(j):
            @pl.when(jnp.logical_not(more))
            def _():
                b_all[me, :, pl.ds(offs[j], widths[j])] = xb[:, pl.ds(offs[j], widths[j])]
                ag_first(b_all, j, x_specs[j])

        rs_drain(final2, send_rows)

        @pl.when(more)
        def _():
            front(layer + 1)
        return carry

    lax.fori_loop(0, layers, layer_body, 0)

    def put(j):
        cols = pl.ds(offs[j], widths[j])
        pltpu.make_async_copy(b_all.at[:, :, cols], x_out.at[:, :, cols], out_sem.at[j]).start()

    all_gather(b_all, x_specs, put, started=True)
    for j in range(chunks):
        cols = pl.ds(offs[j], widths[j])
        pltpu.make_async_copy(b_all.at[:, :, cols], x_out.at[:, :, cols], out_sem.at[j]).wait()


def copy_kernel(split, x_in, c_in, k_in, x_out, c_out, k_out, x_buf, c_buf, k_buf, in_sem, out_sem):
    size = x_in.shape[0] // split
    parts = [(x_in.at[i * size:(i + 1) * size], x_buf.at[i * size:(i + 1) * size], x_out.at[i * size:(i + 1) * size])
             for i in range(split)]
    parts += [(c_in, c_buf, c_out), (k_in, k_buf, k_out)]
    loads = [pltpu.make_async_copy(src, buf, in_sem.at[i]) for i, (src, buf, _) in enumerate(parts)]
    stores = [pltpu.make_async_copy(buf, dst, out_sem.at[i]) for i, (_, buf, dst) in enumerate(parts)]
    for load in loads:
        load.start()
    for load, store in zip(loads, stores):
        load.wait()
        store.start()
    for store in stores:
        store.wait()


def solution(mesh):
    tp = mesh.shape['tp']
    cache_spec = P(None, 'dp', None, None)
    head_spec = P(None, None, 'tp', None)
    weight_specs = (P(), P(), P(), P(), P(), head_spec, head_spec, head_spec, P(None, 'tp', None, None), P(), P(None, None, 'tp'), P(None, None, 'tp'), P(None, 'tp', None))
    in_specs = (P('dp', None), P('dp'), cache_spec, cache_spec) + weight_specs
    out_specs = (P('dp', None), P(None, 'dp', None), P(None, 'dp', None))

    def device_body(x_in, pos_ids, ckv_cache, kpe_cache, attn_gain, w_dq, q_gain, w_dkv, kv_gain, w_uq, w_uk, w_uv, w_o,
                    mlp_gain, w_gate, w_up, w_down):
        batch, model = x_in.shape
        layers, _, keys, latent = ckv_cache.shape
        rope = kpe_cache.shape[-1]
        lora = w_dq.shape[-1]
        heads, per = w_uq.shape[2:]
        nope = w_uk.shape[-1]
        ffn = w_gate.shape[-1]
        rows = batch // tp
        kc, slots, gchunks, direct, seqs, cslots = 512, 3, 4, 0, rows, batch // 2 // rows
        widths = [model * part_w // 28 for part_w in (3, 7, 7, 7, 4)]
        chunks = len(widths)
        hb = pl.BlockSpec(memory_space=pl.ANY)
        dma = pltpu.SemaphoreType.DMA
        qw = lora + latent + 2 * rope
        scratch = [
            pltpu.VMEM((1, batch), jnp.int32),
            pltpu.VMEM((layers, model), BF16),
            pltpu.VMEM((layers, model), BF16),
            pltpu.VMEM((layers, lora), BF16),
            pltpu.VMEM((layers, latent), BF16),
            pltpu.VMEM((batch, heads * rope), F32),
            pltpu.VMEM((batch, heads * rope), F32),
            pltpu.VMEM((batch, keys), jnp.int32),
            pltpu.VMEM((rows, model), BF16),
            pltpu.VMEM((rows, model), BF16),
            pltpu.VMEM((2, rows, model // 2), BF16),
            pltpu.VMEM((tp, rows, model), BF16),
            pltpu.VMEM((tp, rows, qw), BF16),
            pltpu.VMEM((tp, rows, lora + latent + 2 * rope), F32),
            pltpu.VMEM((tp, rows, lora + latent + 2 * rope), F32),
            pltpu.VMEM((heads, batch, latent), BF16),
            pltpu.VMEM((heads, batch, 2 * rope), BF16),
            pltpu.VMEM((heads, batch // 2, latent), BF16),
            pltpu.VMEM((heads, batch // 2, 2 * rope), BF16),
            pltpu.VMEM((heads, batch, latent), BF16),
            pltpu.VMEM((heads, batch // 2, latent), BF16),
            pltpu.VMEM((batch, heads * nope), BF16),
            pltpu.VMEM((latent * heads, nope), F32),
            pltpu.VMEM((batch, ffn), BF16),
            pltpu.VMEM((tp // 2, 2, rows, model), BF16),
            pltpu.VMEM((tp // 2, rows, model), BF16),
            pltpu.VMEM((2, rows, model // 2), BF16),
            pltpu.VMEM((2, rows, model // 2), BF16),
            pltpu.VMEM((2, rows, model), BF16),
            pltpu.VMEM((slots, kc, lora), BF16),
            pltpu.VMEM((slots, latent + rope, kc), BF16),
            pltpu.VMEM((heads * per, lora), BF16),
            pltpu.VMEM((latent * heads, nope), BF16),
            pltpu.VMEM((latent * heads, nope), BF16),
            pltpu.VMEM((heads * nope, model), BF16),
            pltpu.VMEM((2 * ffn, model), BF16),
            pltpu.VMEM((ffn, model), BF16),
            pltpu.VMEM((cslots, seqs, keys, latent), BF16),
            pltpu.VMEM((cslots, seqs, rope, keys), BF16),
            pltpu.VMEM((2 * heads * seqs, keys), F32),
            pltpu.VMEM((rope, batch), BF16),
            dma((2,)), dma((5,)), dma((2, 6)), dma((2, heads + 1)), dma((2, batch // 2 // seqs)), dma((slots,)), dma((slots,)), dma((7,)), dma((2, cslots)), dma((max(gchunks, chunks),)),
            dma((max(gchunks, chunks), 9)), dma((max(gchunks, chunks), 9)), dma((chunks, 7)), dma((chunks, 7)),
        ]
        cfg = dict(tp=tp, layers=layers, heads=heads, kc=kc, slots=slots, widths=widths, seqs=seqs, cslots=cslots, gchunks=gchunks, direct=direct)
        call = pl.pallas_call(
            functools.partial(step_kernel, cfg),
            out_shape=(jax.ShapeDtypeStruct((tp, rows, model), BF16),
                       jax.ShapeDtypeStruct((layers, tp, rows, latent), BF16),
                       jax.ShapeDtypeStruct((layers, rope, batch), BF16)),
            in_specs=[hb] * 17,
            out_specs=(hb, hb, hb),
            scratch_shapes=scratch,
            compiler_params=pltpu.CompilerParams(collective_id=0, has_side_effects=True, vmem_limit_bytes=67043328),
            name='decode_step',
        )
        x_o, c_o, k_o = call(
            x_in.reshape(tp, rows, model), pos_ids.reshape(1, batch), attn_gain, mlp_gain, q_gain, kv_gain,
            w_dq, w_dkv.transpose(0, 2, 1), w_uq.transpose(0, 2, 3, 1).reshape(layers, heads * per, lora),
            w_uk.reshape(layers, latent * heads, nope), w_uv.reshape(layers, latent * heads, nope),
            w_o.reshape(layers, heads * nope, model),
            w_gate.transpose(0, 2, 1), w_up.transpose(0, 2, 1), w_down,
            ckv_cache, kpe_cache.transpose(0, 1, 3, 2))
        split = 4
        x_o, c_o, k_o = pl.pallas_call(
            functools.partial(copy_kernel, split),
            out_shape=tuple(jax.ShapeDtypeStruct(v.shape, v.dtype) for v in (x_o, c_o, k_o)),
            in_specs=[hb] * 3,
            out_specs=(hb, hb, hb),
            scratch_shapes=[pltpu.VMEM(v.shape, v.dtype) for v in (x_o, c_o, k_o)] + [dma((split + 2,)), dma((split + 2,))],
            name='copy_out',
        )(x_o, c_o, k_o)
        return x_o.reshape(batch, model), c_o.reshape(layers, batch, latent), k_o.transpose(0, 2, 1)

    return jax.shard_map(device_body, mesh=mesh, in_specs=in_specs, out_specs=out_specs, check_vma=False)
```
